32 devices in a mesh: tp: 8 (over z, y), dp: 4 (over x, core).
Axes of the slice: x: 2, y: 2, z: 4, core: 2. Of those that a mesh axis runs over, the one named last changes fastest.
Arguments:
- normed: bfloat16 [1024, 4096], P(('dp', 'tp')), may hold values from -6 to 6
- cotangent: bfloat16 [1024, 8192], P('dp', 'tp'), may hold values from -1.5 to 1.5
- weight_tiles: bfloat16 [2, 2048, 128, 128], P(None, 'tp'), may hold values from -0.09375 to 0.09375
- slot_tile: int32 [2048], replicated, may hold values from 0 to 2047, as said below
Outputs:
- hidden: bfloat16 [1024, 8192], P('dp', 'tp')
- d_normed: bfloat16 [1024, 4096], P(('dp', 'tp'))
- grad_tiles: float32 [2, 2048, 128, 128], P(None, 'tp', 'dp')
The draws below stay inside these ranges and needn't reach their ends.
Inputs may be any that keep to these rules, and one draw needn't show every extreme that they name: `slot_tile`: A permutation of 0 to 2047. Position p belongs to owner p // 256 at slot p % 256. Each owner holds 24 to 40 tiles of the tile columns t * 8 to (t + 1) * 8 - 1 of each index t of tp; in every draw some owner holds exactly 40 for some t.
All inputs are finite; a program needn't handle non-finite values.
Results may differ from the reference program's by a relative error of at most 0.018.
Values may be sent and summed in bfloat16 or wider, within the bound.
A program may use at most 128 MiB of HBM per device.

```python
import jax
import jax.numpy as jnp
from jax import lax

D = 4096
FW = 8192
TILE = 128
TOKENS = 1024
TR = 32
TC = 64
TPC = 8
NTILES = 2048
OWN = 256
N_DP = 4


def tile_layout(key):
    groups = TC // TPC
    owned_count = OWN
    base_count = owned_count // groups
    swing_count = base_count // 4
    key_offset, key_cons, key_owner = jax.random.split(jax.random.fold_in(key, 7), 3)
    offset_draw = jax.random.randint(key_offset, (), 0, groups)
    owner_axis = jnp.arange(groups)[:, None]
    cons_axis = jnp.arange(groups)[None, :]
    phase_step = (cons_axis - owner_axis + offset_draw) % groups
    counts = base_count + swing_count * (1 - 2 * (phase_step % 2))
    list_ends = jnp.cumsum(counts, axis=0)
    starts = list_ends - counts
    rank_ix = jnp.arange(owned_count)
    owner_of = jnp.sum((rank_ix[None, :, None] >= list_ends.T[:, None, :]).astype(jnp.int32), axis=2)
    index_in = rank_ix[None, :] - jnp.take_along_axis(starts.T, owner_of, axis=1)
    local_perm = jax.vmap(lambda sub: jax.random.permutation(sub, owned_count))(jax.random.split(key_cons, groups))
    cons_rows = jnp.broadcast_to(jnp.arange(groups)[:, None], (groups, owned_count))
    tile_row = local_perm // TPC
    tile_col = cons_rows * TPC + local_perm % TPC
    tile_id = (tile_row * TC + tile_col).astype(jnp.int32)
    offsets = jnp.cumsum(counts, axis=1) - counts
    pre_slot = offsets[owner_of, cons_rows] + index_in
    shuffles = jax.vmap(lambda sub: jax.random.permutation(sub, owned_count))(jax.random.split(key_owner, groups))
    slot_ix = shuffles[owner_of, pre_slot].astype(jnp.int32)
    slot_table = jnp.zeros((NTILES,), jnp.int32).at[(owner_of * owned_count + slot_ix).reshape(-1)].set(tile_id.reshape(-1))
    return slot_table


def draw_slot_tile(key, part):
    return tile_layout(key)


def shard_levels(stream_key, shape, cuts, low, high):
    factor_of, own = 1.0, jax.random.fold_in(stream_key, 6)
    for dim, shards_of in cuts:
        steps = jnp.exp(jax.random.uniform(jax.random.fold_in(own, dim), (shards_of,), jnp.float32, low / len(cuts), high / len(cuts)))
        factor_of = factor_of * jnp.repeat(steps, shape[dim] // shards_of).reshape([-1 if axis == dim else 1 for axis in range(len(shape))])
    return factor_of


def scatter_about(stream_key, shape, scale, reach, shards=(), kind=jnp.bfloat16):
    drawn = scale * jax.random.normal(stream_key, shape, jnp.float32)
    if shards:
        drawn = drawn * shard_levels(stream_key, shape, shards, -0.22, 0.18)
    return jnp.clip(drawn, -reach, reach).astype(kind)


def setup_inputs(seed: int = 0) -> dict:
    splits = jax.random.split(jax.random.key(seed), 5)
    normed = scatter_about(splits[0], (TOKENS, D), 1.0, 6.0, ((0, 32),))
    cotangent = scatter_about(splits[1], (TOKENS, FW), (8.0 / TOKENS ** 0.5), 1.5, ((0, 4), (1, 8)))
    weight_tiles = scatter_about(splits[2], (2, NTILES, TILE, TILE), D ** -0.5, 0.09375, ((1, 8),))
    slot_tile = draw_slot_tile(jax.random.fold_in(splits[4], 71), 0)
    return {"normed": normed, "cotangent": cotangent, "weight_tiles": weight_tiles, "slot_tile": slot_tile}


def reference(normed, cotangent, weight_tiles, slot_tile):
    by_number = jnp.zeros_like(weight_tiles).at[:, slot_tile].set(weight_tiles)
    weights = by_number.reshape(2, TR, TC, TILE, TILE).transpose(0, 1, 3, 2, 4).reshape(2, D, FW)
    gate_proj = jnp.dot(normed, weights[0], preferred_element_type=jnp.float32)
    up_proj = jnp.dot(normed, weights[1], preferred_element_type=jnp.float32)
    sigmoid_gate = jax.nn.sigmoid(gate_proj)
    act_gate = gate_proj * sigmoid_gate
    hidden = (act_gate * up_proj).astype(jnp.bfloat16)
    cot_full = cotangent.astype(jnp.float32)
    grad_gate = (cot_full * up_proj * (sigmoid_gate * (1.0 + gate_proj * (1.0 - sigmoid_gate)))).astype(jnp.bfloat16)
    grad_up = (cot_full * act_gate).astype(jnp.bfloat16)
    d_normed = (jnp.dot(grad_gate, weights[0].T, preferred_element_type=jnp.float32)
                + jnp.dot(grad_up, weights[1].T, preferred_element_type=jnp.float32)).astype(jnp.bfloat16)

    def replica(running, group_block):
        rows_in, rows_gate, rows_up = group_block
        part_gate = jnp.dot(rows_in.T, rows_gate, preferred_element_type=jnp.float32).astype(jnp.bfloat16)
        part_up = jnp.dot(rows_in.T, rows_up, preferred_element_type=jnp.float32).astype(jnp.bfloat16)
        stacked = lax.optimization_barrier(jnp.stack([part_gate, part_up]))
        return running + stacked.astype(jnp.float32), None

    start_sum = jnp.zeros((2, D, FW), jnp.float32)
    summed, _ = lax.scan(replica, start_sum, (normed.reshape(N_DP, -1, D), grad_gate.reshape(N_DP, -1, FW), grad_up.reshape(N_DP, -1, FW)))
    grad_tiled = summed.reshape(2, TR, TILE, TC, TILE).transpose(0, 1, 3, 2, 4).reshape(2, TR * TC, TILE, TILE)
    grad_tiles = grad_tiled[:, slot_tile]
    return hidden, d_normed, grad_tiles
```

```python
import functools

import jax
import jax.numpy as jnp
from jax import lax
from jax.experimental import pallas as pl
from jax.experimental.pallas import tpu as pltpu
from jax.sharding import PartitionSpec as P

MESH = pl.DeviceIdType.MESH
VMEM_LIMIT = 67_043_328
CORES = 2


def ring_width(n):
    width = 2
    while 4 * width * width <= n:
        width *= 2
    return width


def ring_pos(index, n):
    y_size = ring_width(n)
    z, y = lax.div(index, y_size), lax.rem(index, y_size)
    inner = lax.div(y + y_size - 1, y_size)
    odd = lax.rem(z, 2)
    snake = z * (y_size - 1) + (1 - odd) * (y - 1) + odd * (y_size - 1 - y)
    return inner * snake + (1 - inner) * (n - 1 - z)


def ring_index(pos, n):
    y_size = ring_width(n)
    z_size = n // y_size
    back = lax.div(pos, n - z_size)
    z = lax.div(pos, y_size - 1)
    k = lax.rem(pos, y_size - 1)
    odd = lax.rem(z, 2)
    y = (1 - odd) * (k + 1) + odd * (y_size - 1 - k)
    return (1 - back) * (z * y_size + y) + back * (n - 1 - pos) * y_size


class Ring:
    def __init__(self, n):
        self.n = n
        self.half = n // 2
        self.pos = ring_pos(lax.axis_index("tp"), n)

    def at(self, offset):
        return ring_index(lax.rem(self.pos + offset + self.n, self.n), self.n)


def hops(ring, way, piece):
    return ring.half if way == piece else ring.half - 1


def step_of(way):
    return 1 - 2 * way


def build_tables(slot_tile, me, owned, tile_rows, tile_cols, n, list_len):
    cols_dev = tile_cols // n
    mine = lax.dynamic_slice(slot_tile, (me * owned,), (owned,))
    row, col = mine // tile_cols, mine % tile_cols
    group = col // cols_dev
    local_col = col % cols_dev
    same = group[None, :] == group[:, None]
    places = jnp.arange(n * list_len, dtype=jnp.int32)
    slots = jnp.arange(owned, dtype=jnp.int32)

    def build(key, sub, n_sub):
        less = same & (key[None, :] < key[:, None])
        pos = jnp.sum(less.astype(jnp.int32), axis=1)
        place = group * list_len + pos
        hit = places[:, None] == place[None, :]

        def pick(value):
            return jnp.sum(jnp.where(hit, value[None, :], 0), axis=1)

        sub_at = pick(sub + 1)
        before = jnp.concatenate([jnp.zeros((1,), jnp.int32), sub_at[:-1]])
        keep = (sub_at == before) & (places % list_len > 0)
        buckets = jnp.arange(n * n_sub, dtype=jnp.int32)
        in_bucket = buckets[:, None] == (group * n_sub + sub)[None, :]
        last = jnp.max(jnp.where(in_bucket, pos[None, :] + 1, 0), axis=1)
        return pick(slots), pick(row), pick(local_col), keep.astype(jnp.int32), last, place

    by_col = build(col * tile_rows + row, local_col, cols_dev)
    by_row = build(row * tile_cols + col, row, tile_rows)
    return by_col, by_row


def forward_kernel(
    dims, slot_tab, row_tab, keep_tab, last_tab, x_ref, cot_ref, w_ref,
    hidden_ref, grads_ref, xt_ref,
    xg, ww, buf, part, send, recv, cot, load_sem, ag_send, ag_recv, rs_send, rs_recv,
):
    n, tile_rows, cols_dev, list_len, rows, tile, dp_size = dims
    ring = Ring(n)
    half = ring.half
    me = lax.axis_index("tp")
    piece_cols = cols_dev // 2
    piece_rows = tile_rows // 2

    own_rows = pl.ds(pl.multiple_of(me * rows, rows), rows)
    loads = [
        pltpu.make_async_copy(x_ref, xg.at[:, own_rows, :], load_sem.at[0]),
        pltpu.make_async_copy(w_ref.at[0], ww.at[:, :, pl.ds(0, tile)], load_sem.at[1]),
        pltpu.make_async_copy(w_ref.at[1], ww.at[:, :, pl.ds(tile, tile)], load_sem.at[2]),
        pltpu.make_async_copy(cot_ref, cot, load_sem.at[3]),
    ]
    for load in loads:
        load.start()

    barrier = pltpu.get_barrier_semaphore()
    for offset in (1, -1):
        pl.semaphore_signal(
            barrier, inc=1, device_id={"tp": ring.at(offset)}, device_id_type=MESH
        )
    pl.semaphore_wait(barrier, 2)
    loads[0].wait()

    def token_copy(way, piece, hop):
        shard = ring.at(-step_of(way) * hop)
        view = xg.at[
            pl.ds(piece * piece_rows, piece_rows),
            pl.ds(pl.multiple_of(shard * rows, rows), rows),
            :,
        ]
        return pltpu.make_async_remote_copy(
            src_ref=view, dst_ref=view,
            send_sem=ag_send.at[way, piece, hop], recv_sem=ag_recv.at[way, piece, hop],
            device_id={"tp": ring.at(step_of(way))}, device_id_type=MESH,
        )

    lanes = [(way, piece) for piece in range(2) for way in range(2)]
    for way, piece in lanes:
        token_copy(way, piece, 0).start()
    for hop in range(half):
        for way, piece in lanes:
            if hop < hops(ring, way, piece):
                token_copy(way, piece, hop).wait_recv()
                if hop + 1 < hops(ring, way, piece):
                    token_copy(way, piece, hop + 1).start()
    loads[1].wait()
    loads[2].wait()

    buf[0] = jnp.zeros(buf.shape[1:], buf.dtype)

    def compute(which, dest):
        def tile_step(j, carry):
            at = dest * list_len + j
            term = jnp.dot(
                xg[row_tab[at]], ww[slot_tab[at]], preferred_element_type=jnp.float32
            )
            buf[j + 1] = term + jnp.where(keep_tab[at] > 0, buf[j], 0.0)
            return carry

        lax.fori_loop(0, list_len, tile_step, 0)

        def column(c, carry):
            part[which, c] = buf[last_tab[dest * cols_dev + c]]
            return carry

        lax.fori_loop(0, cols_dev, column, 0)

    def sum_copy(way, piece, hop):
        return pltpu.make_async_remote_copy(
            src_ref=send.at[way, piece, hop], dst_ref=recv.at[way, piece, hop],
            send_sem=rs_send.at[way, piece, hop], recv_sem=rs_recv.at[way, piece, hop],
            device_id={"tp": ring.at(step_of(way))}, device_id_type=MESH,
        )

    def first_hop(way, piece):
        return half - hops(ring, way, piece)

    def push(which, way, piece, hop):
        fresh = hop == first_hop(way, piece)
        if not fresh:
            sum_copy(way, piece, hop - 1).wait_recv()

        def column(c, carry):
            value = part[which, piece * piece_cols + c]
            if not fresh:
                value = value + recv[way, piece, hop - 1, c].astype(jnp.float32)
            send[way, piece, hop, c] = value.astype(jnp.bfloat16)
            return carry

        lax.fori_loop(0, piece_cols, column, 0)
        sum_copy(way, piece, hop).start()

    compute(0, ring.at(half))
    push(0, 0, 0, 0)
    push(0, 1, 1, 0)

    for hop in range(1, half):
        compute(0, ring.at(half - hop))
        compute(1, ring.at(hop - half))
        push(0, 0, 1, hop)
        push(1, 1, 0, hop)
        push(0, 0, 0, hop)
        push(1, 1, 1, hop)

    compute(0, me)

    band = tile // dp_size
    parts = dp_size // CORES
    order = lax.broadcasted_iota(jnp.int32, (tile, tile), 0)
    source = lax.broadcasted_iota(jnp.int32, (tile, tile), 1)
    core = order // (parts * band)
    x_part = order // band % parts
    perm = (source == (x_part * CORES + core) * band + order % band).astype(jnp.bfloat16)

    def transpose_block(r, carry):
        turned = lax.dot_general(
            perm, xg[r], (((1,), (1,)), ((), ())), preferred_element_type=jnp.float32
        ).astype(jnp.bfloat16)
        for c in range(CORES):
            xt_ref[c, r] = turned[c * (tile // CORES) : (c + 1) * (tile // CORES)]
        return carry

    lax.fori_loop(0, tile_rows, transpose_block, 0)
    loads[3].wait()

    for piece in (1, 0):
        for way in range(2):
            sum_copy(way, piece, half - 1).wait_recv()
        for k in range(piece_cols):
            c = piece * piece_cols + k
            total = (
                part[0, c]
                + recv[0, piece, half - 1, k].astype(jnp.float32)
                + recv[1, piece, half - 1, k].astype(jnp.float32)
            )
            gate, up = total[:, :tile], total[:, tile:]
            s = jax.nn.sigmoid(gate)
            act = gate * s
            cotangent = cot[:, c * tile : (c + 1) * tile].astype(jnp.float32)
            hidden_ref[:, c * tile : (c + 1) * tile] = (act * up).astype(jnp.bfloat16)
            grads_ref[c, :, :tile] = (
                cotangent * up * (s * (1.0 + gate * (1.0 - s)))
            ).astype(jnp.bfloat16)
            grads_ref[c, :, tile:] = (cotangent * act).astype(jnp.bfloat16)

    for way, piece in lanes:
        for hop in range(hops(ring, way, piece)):
            token_copy(way, piece, hop).wait_send()
        for hop in range(first_hop(way, piece), half):
            sum_copy(way, piece, hop).wait_send()


def forward(tables, x, cotangent, weights, n, list_len, dp_size):
    slot_tab, row_tab, _, keep_tab, last_tab, _ = tables
    tile_rows, rows, tile = x.shape
    tokens, cols = cotangent.shape
    owned = weights.shape[1]
    cols_dev = cols // tile
    half = n // 2
    dims = (n, tile_rows, cols_dev, list_len, rows, tile, dp_size)
    smem = pl.BlockSpec(memory_space=pltpu.SMEM)
    hbm = pl.BlockSpec(memory_space=pl.ANY)
    vmem = pl.BlockSpec(memory_space=pltpu.VMEM)
    slots = (2, 2, half, cols_dev // 2, tokens, 2 * tile)
    return pl.pallas_call(
        functools.partial(forward_kernel, dims),
        name="forward",
        in_specs=[smem] * 4 + [hbm] * 3,
        out_specs=[vmem, vmem, vmem],
        out_shape=[
            jax.ShapeDtypeStruct((tokens, cols), jnp.bfloat16),
            jax.ShapeDtypeStruct((cols_dev, tokens, 2 * tile), jnp.bfloat16),
            jax.ShapeDtypeStruct((CORES, tile_rows, tile // CORES, tokens), jnp.bfloat16),
        ],
        scratch_shapes=[
            pltpu.VMEM((tile_rows, tokens, tile), jnp.bfloat16),
            pltpu.VMEM((owned, tile, 2 * tile), jnp.bfloat16),
            pltpu.VMEM((list_len + 1, tokens, 2 * tile), jnp.float32),
            pltpu.VMEM((2, cols_dev, tokens, 2 * tile), jnp.float32),
            pltpu.VMEM(slots, jnp.bfloat16),
            pltpu.VMEM(slots, jnp.bfloat16),
            pltpu.VMEM((tokens, cols), jnp.bfloat16),
            pltpu.SemaphoreType.DMA((4,)),
            pltpu.SemaphoreType.DMA((2, 2, half)),
            pltpu.SemaphoreType.DMA((2, 2, half)),
            pltpu.SemaphoreType.DMA((2, 2, half)),
            pltpu.SemaphoreType.DMA((2, 2, half)),
        ],
        compiler_params=pltpu.CompilerParams(
            collective_id=0, has_side_effects=True, vmem_limit_bytes=VMEM_LIMIT
        ),
    )(slot_tab, row_tab, keep_tab, last_tab, x, cotangent, weights)


def backward_kernel(
    dims, big, slot_tab, row_tab, col_tab, keep_tab, last_tab, grads_ref, xt_ref, w_ref,
    d_ref, parts_ref, *rest,
):
    n, tile_rows, cols_dev, list_len, rows, tokens, tile, dp_size = dims
    (gall, gw, ww, xt, buf, dx, stage, send, recv,
     load_sem, work_sem, g_send, g_recv, p_send, p_recv, t_sem,
     x_send, x_recv, x_local, rs_send, rs_recv) = rest
    ring = Ring(n)
    half = ring.half
    me = lax.axis_index("tp")
    me_dp = lax.axis_index("dp")
    core, x_part = lax.rem(me_dp, CORES), lax.div(me_dp, CORES)
    n_parts = dp_size // CORES
    band = tile // dp_size
    piece_cols = cols_dev // 2
    piece_rows = tile_rows // 2
    n_stage = stage.shape[0]
    partner = {"dp": x_part * CORES + 1 - core}

    own_cols = pl.ds(pl.multiple_of(me * cols_dev, cols_dev), cols_dev)
    loads = [
        pltpu.make_async_copy(grads_ref, gall.at[0, own_cols], load_sem.at[0]),
        pltpu.make_async_copy(xt_ref.at[core], xt.at[0], load_sem.at[1]),
        pltpu.make_async_copy(w_ref.at[0], ww.at[:, :, pl.ds(0, tile)], load_sem.at[2]),
        pltpu.make_async_copy(w_ref.at[1], ww.at[:, :, pl.ds(tile, tile)], load_sem.at[3]),
    ]
    for load in loads:
        load.start()

    barrier = pltpu.get_barrier_semaphore()
    for offset in (1, -1):
        pl.semaphore_signal(
            barrier, inc=1, device_id={"tp": ring.at(offset)}, device_id_type=MESH
        )
    pl.semaphore_signal(barrier, inc=1, device_id=partner, device_id_type=MESH)

    def x_device(off):
        return {"dp": lax.rem(x_part + off, n_parts) * CORES + core}

    for off in range(1, n_parts):
        pl.semaphore_signal(barrier, inc=1, device_id=x_device(off), device_id_type=MESH)
    pl.semaphore_wait(barrier, 3 + n_parts - 1)

    turned = pltpu.make_async_remote_copy(
        src_ref=xt_ref.at[1 - core], dst_ref=xt.at[1],
        send_sem=t_sem.at[0], recv_sem=t_sem.at[1],
        device_id=partner, device_id_type=MESH,
    )

    def piece_view(side, shard, piece):
        start = pl.multiple_of(shard * cols_dev + piece * piece_cols, piece_cols)
        return gall.at[side, pl.ds(start, piece_cols)]

    def grad_copy(way, piece, hop):
        view = piece_view(0, ring.at(-step_of(way) * hop), piece)
        return pltpu.make_async_remote_copy(
            src_ref=view, dst_ref=view,
            send_sem=g_send.at[way, piece, hop], recv_sem=g_recv.at[way, piece, hop],
            device_id={"tp": ring.at(step_of(way))}, device_id_type=MESH,
        )

    def group_number(offset):
        return offset % n

    def pair_copy(offset, piece):
        shard = ring.at(offset)
        g = group_number(offset)
        return pltpu.make_async_remote_copy(
            src_ref=piece_view(0, shard, piece), dst_ref=piece_view(1, shard, piece),
            send_sem=p_send.at[g, piece], recv_sem=p_recv.at[g, piece],
            device_id=partner, device_id_type=MESH,
        )

    def x_copy(i, offset, off):
        dest = lax.rem(x_part + off, n_parts)
        shard = ring.at(offset)
        return pltpu.make_async_remote_copy(
            src_ref=stage.at[i % n_stage, dest],
            dst_ref=parts_ref.at[
                x_part, pl.ds(pl.multiple_of(shard * list_len, list_len), list_len)
            ],
            send_sem=x_send.at[i, off - 1], recv_sem=x_recv.at[i, off - 1],
            device_id=x_device(off), device_id_type=MESH,
        )

    def keep_copy(i, offset):
        shard = ring.at(offset)
        return pltpu.make_async_copy(
            stage.at[i % n_stage, x_part],
            parts_ref.at[
                x_part, pl.ds(pl.multiple_of(shard * list_len, list_len), list_len)
            ],
            x_local.at[i],
        )

    def finish(i, offset):
        for off in range(1, n_parts):
            x_copy(i, offset, off).wait_send()
        keep_copy(i, offset).wait()

    lanes = [(0, 0), (1, 1), (0, 1), (1, 0)]
    loads[0].wait()
    for way, piece in lanes:
        grad_copy(way, piece, 0).start()
    for piece in range(2):
        pair_copy(0, piece).start()
    turned.start()

    dx[...] = jnp.zeros(dx.shape, dx.dtype)
    buf[0] = jnp.zeros(buf.shape[1:], buf.dtype)
    for load in loads[1:]:
        load.wait()
    turned.wait()

    done = []

    def process(offset):
        i = len(done)
        shard = ring.at(offset)
        for piece in range(2):
            pair_copy(offset, piece).wait_recv()
        cols = pl.ds(pl.multiple_of(shard * cols_dev, cols_dev), cols_dev)
        fills = [
            pltpu.make_async_copy(gall.at[side, cols], gw.at[side], work_sem.at[side])
            for side in range(2)
        ]
        for fill in fills:
            fill.start()
        if i >= n_stage:
            finish(i - n_stage, done[i - n_stage])
        for fill in fills:
            fill.wait()
        slot = i % n_stage

        def outer(j, carry):
            at = shard * list_len + j
            r, c = row_tab[at], col_tab[at]
            value = jnp.dot(
                xt[0, r], gw[0, c], preferred_element_type=jnp.float32
            ) + jnp.dot(xt[1, r], gw[1, c], preferred_element_type=jnp.float32)
            for k in range(n_parts):
                stage[slot, k, j] = value[k * band : (k + 1) * band].astype(jnp.bfloat16)
            return carry

        lax.fori_loop(0, list_len, outer, 0)
        for off in range(1, n_parts):
            x_copy(i, offset, off).start()
        keep_copy(i, offset).start()

        def back(j, carry):
            at = shard * list_len + j
            term = lax.dot_general(
                gw[0, col_tab[at]], ww[slot_tab[at]], (((1,), (1,)), ((), ())),
                preferred_element_type=jnp.float32,
            )
            buf[j + 1] = term + jnp.where(keep_tab[at] > 0, buf[j], 0.0)
            return carry

        lax.fori_loop(0, list_len, back, 0)

        def add_row(r, carry):
            dx[r] += buf[last_tab[shard * tile_rows + r]]
            return carry

        lax.fori_loop(0, tile_rows, add_row, 0)
        done.append(offset)

    def arrive(way, piece, hop):
        if hop >= hops(ring, way, piece):
            return
        grad_copy(way, piece, hop).wait_recv()
        if hop + 1 < hops(ring, way, piece):
            grad_copy(way, piece, hop + 1).start()
        pair_copy(-step_of(way) * (hop + 1), piece).start()

    process(0)
    for hop in range(half):
        arrive(0, 0, hop)
        arrive(1, 1, hop)
        if hop > 0:
            process(-hop)
        arrive(0, 1, hop)
        arrive(1, 0, hop)
        if hop > 0:
            process(hop)
    process(half)

    def sum_copy(way, piece, hop):
        return pltpu.make_async_remote_copy(
            src_ref=send.at[way, piece, hop], dst_ref=recv.at[way, piece, hop],
            send_sem=rs_send.at[way, piece, hop], recv_sem=rs_recv.at[way, piece, hop],
            device_id={"tp": ring.at(step_of(way))}, device_id_type=MESH,
        )

    def first_hop(way, piece):
        return half - hops(ring, way, piece)

    def own_term(dest, piece):
        return dx[
            pl.ds(piece * piece_rows, piece_rows),
            pl.ds(pl.multiple_of(dest * rows, rows), rows),
            :,
        ]

    def push(way, piece, hop):
        value = own_term(ring.at(step_of(way) * (half - hop)), piece)
        if hop > first_hop(way, piece):
            sum_copy(way, piece, hop - 1).wait_recv()
            value = value + recv[way, piece, hop - 1].astype(jnp.float32)
        send[way, piece, hop] = value.astype(jnp.bfloat16)
        sum_copy(way, piece, hop).start()

    push(0, 0, 0)
    push(1, 1, 0)
    for hop in range(1, half):
        for way, piece in ((0, 1), (1, 0), (0, 0), (1, 1)):
            push(way, piece, hop)
    for piece in range(2):
        for way in range(2):
            sum_copy(way, piece, half - 1).wait_recv()
        d_ref[pl.ds(piece * piece_rows, piece_rows)] = (
            own_term(me, piece)
            + recv[0, piece, half - 1].astype(jnp.float32)
            + recv[1, piece, half - 1].astype(jnp.float32)
        ).astype(jnp.bfloat16)

    for i in range(max(0, n - n_stage), n):
        finish(i, done[i])
    for i in range(n):
        for off in range(1, n_parts):
            x_copy(i, done[i], off).wait_recv()
    for way, piece in lanes:
        for hop in range(hops(ring, way, piece)):
            grad_copy(way, piece, hop).wait_send()
        for hop in range(first_hop(way, piece), half):
            sum_copy(way, piece, hop).wait_send()
    for offset in done:
        for piece in range(2):
            pair_copy(offset, piece).wait_send()


def backward(tables, grads, xt, weights, n, list_len, rows, dp_size):
    slot_tab, row_tab, col_tab, keep_tab, last_tab, _ = tables
    _, tile_rows, half_tile, tokens = xt.shape
    cols_dev, _, pair = grads.shape
    tile = pair // 2
    owned = weights.shape[1]
    half = n // 2
    band = tile // dp_size
    n_parts = dp_size // CORES
    n_stage = 4
    dims = (n, tile_rows, cols_dev, list_len, rows, tokens, tile, dp_size)
    smem = pl.BlockSpec(memory_space=pltpu.SMEM)
    hbm = pl.BlockSpec(memory_space=pl.ANY)
    vmem = pl.BlockSpec(memory_space=pltpu.VMEM)
    slots = (2, 2, half, tile_rows // 2, rows, tile)
    gall_shape = (2, n * cols_dev, tokens, pair)
    big = 2 * n * cols_dev * tokens * pair * 2 > 24 * 2**20
    sem = pltpu.SemaphoreType.DMA
    out_specs = [vmem, hbm]
    out_shape = [
        jax.ShapeDtypeStruct((tile_rows, rows, tile), jnp.bfloat16),
        jax.ShapeDtypeStruct((n_parts, n * list_len, band, pair), jnp.bfloat16),
    ]
    scratch = []
    if big:
        out_specs.append(hbm)
        out_shape.append(jax.ShapeDtypeStruct(gall_shape, jnp.bfloat16))
    else:
        scratch.append(pltpu.VMEM(gall_shape, jnp.bfloat16))
    scratch += [
        pltpu.VMEM((2, cols_dev, tokens, pair), jnp.bfloat16),
        pltpu.VMEM((owned, tile, pair), jnp.bfloat16),
        pltpu.VMEM((2, tile_rows, half_tile, tokens), jnp.bfloat16),
        pltpu.VMEM((list_len + 1, tokens, tile), jnp.float32),
        pltpu.VMEM((tile_rows, tokens, tile), jnp.float32),
        pltpu.VMEM((n_stage, n_parts, list_len, band, pair), jnp.bfloat16),
        pltpu.VMEM(slots, jnp.bfloat16),
        pltpu.VMEM(slots, jnp.bfloat16),
        sem((4,)), sem((2,)),
        sem((2, 2, half)), sem((2, 2, half)),
        sem((n, 2)), sem((n, 2)), sem((2,)),
        sem((n, n_parts - 1)), sem((n, n_parts - 1)), sem((n,)),
        sem((2, 2, half)), sem((2, 2, half)),
    ]
    results = pl.pallas_call(
        functools.partial(backward_kernel, dims, big),
        name="backward",
        in_specs=[smem] * 5 + [hbm] * 3,
        out_specs=out_specs,
        out_shape=out_shape,
        scratch_shapes=scratch,
        compiler_params=pltpu.CompilerParams(
            collective_id=1, has_side_effects=True, vmem_limit_bytes=VMEM_LIMIT
        ),
    )(slot_tab, row_tab, col_tab, keep_tab, last_tab, grads, xt, weights)
    return results[0], results[1]


def finish_kernel(place_ref, parts_ref, out_ref):
    n_parts = parts_ref.shape[0]
    _, chunk, _, tile = out_ref.shape
    base = pl.program_id(0) * chunk

    def one(p, carry):
        at = place_ref[base + p]
        total = parts_ref[0, at].astype(jnp.float32)
        for k in range(1, n_parts):
            total = total + parts_ref[k, at].astype(jnp.float32)
        out_ref[0, p] = total[:, :tile]
        out_ref[1, p] = total[:, tile:]
        return carry

    lax.fori_loop(0, chunk, one, 0)


def finish_sum(place, parts):
    owned = place.shape[0]
    n_parts, listed, band, pair = parts.shape
    tile = pair // 2
    steps = 8
    return pl.pallas_call(
        finish_kernel,
        name="finish",
        grid=(steps,),
        in_specs=[
            pl.BlockSpec(memory_space=pltpu.SMEM),
            pl.BlockSpec((n_parts, listed, band, pair), lambda i: (0, 0, 0, 0)),
        ],
        out_specs=pl.BlockSpec((2, owned // steps, band, tile), lambda i: (0, i, 0, 0)),
        out_shape=jax.ShapeDtypeStruct((2, owned, band, tile), jnp.float32),
        compiler_params=pltpu.CompilerParams(vmem_limit_bytes=VMEM_LIMIT),
    )(place, parts)


def local(normed, cotangent, weight_tiles, slot_tile):
    n = lax.axis_size("tp")
    dp_size = lax.axis_size("dp")
    me = lax.axis_index("tp")
    rows, width = normed.shape
    owned, tile = weight_tiles.shape[1:3]
    tile_rows = width // tile
    tile_cols = cotangent.shape[1] // tile * n
    base_count = owned // n
    list_len = base_count + base_count // 4
    by_col, by_row = build_tables(slot_tile, me, owned, tile_rows, tile_cols, n, list_len)
    x = normed.reshape(rows, tile_rows, tile).transpose(1, 0, 2)
    hidden, grads, xt = forward(by_col, x, cotangent, weight_tiles, n, list_len, dp_size)
    d, parts = backward(by_row, grads, xt, weight_tiles, n, list_len, rows, dp_size)
    grad_tiles = finish_sum(by_row[-1], parts)
    d_normed = d.transpose(1, 0, 2).reshape(rows, width)
    return hidden, d_normed, grad_tiles


def solution(mesh):
    return jax.shard_map(
        local,
        mesh=mesh,
        in_specs=(P(("dp", "tp"), None), P("dp", "tp"), P(None, "tp", None, None), P()),
        out_specs=(P("dp", "tp"), P(("dp", "tp"), None), P(None, "tp", "dp", None)),
        check_vma=False,
    )
```

```python
import functools

import jax
import jax.numpy as jnp
from jax import lax
from jax.experimental import pallas as pl
from jax.experimental.pallas import tpu as pltpu
from jax.sharding import PartitionSpec as P

MESH = pl.DeviceIdType.MESH
VMEM_LIMIT = 67_043_328
CORES = 2


def ring_width(n):
    width = 2
    while 4 * width * width <= n:
        width *= 2
    return width


def ring_pos(index, n):
    y_size = ring_width(n)
    z, y = lax.div(index, y_size), lax.rem(index, y_size)
    inner = lax.div(y + y_size - 1, y_size)
    odd = lax.rem(z, 2)
    snake = z * (y_size - 1) + (1 - odd) * (y - 1) + odd * (y_size - 1 - y)
    return inner * snake + (1 - inner) * (n - 1 - z)


def ring_index(pos, n):
    y_size = ring_width(n)
    z_size = n // y_size
    back = lax.div(pos, n - z_size)
    z = lax.div(pos, y_size - 1)
    k = lax.rem(pos, y_size - 1)
    odd = lax.rem(z, 2)
    y = (1 - odd) * (k + 1) + odd * (y_size - 1 - k)
    return (1 - back) * (z * y_size + y) + back * (n - 1 - pos) * y_size


class Ring:
    def __init__(self, n):
        self.n = n
        self.half = n // 2
        self.pos = ring_pos(lax.axis_index("tp"), n)

    def at(self, offset):
        return ring_index(lax.rem(self.pos + offset + self.n, self.n), self.n)


def hops(ring, way, piece):
    return ring.half if way == piece else ring.half - 1


def step_of(way):
    return 1 - 2 * way


def unrolled(count, body):
    by = 4 if count % 4 == 0 else 2 if count % 2 == 0 else 1

    def steps(i, carry):
        for u in range(by):
            body(i * by + u)
        return carry

    lax.fori_loop(0, count // by, steps, 0)


def build_tables(slot_tile, me, owned, tile_rows, tile_cols, n, list_len):
    cols_dev = tile_cols // n
    mine = lax.dynamic_slice(slot_tile, (me * owned,), (owned,))
    row, col = mine // tile_cols, mine % tile_cols
    group = col // cols_dev
    local_col = col % cols_dev
    same = group[None, :] == group[:, None]
    places = jnp.arange(n * list_len, dtype=jnp.int32)
    slots = jnp.arange(owned, dtype=jnp.int32)

    def build(key, sub, n_sub):
        less = same & (key[None, :] < key[:, None])
        pos = jnp.sum(less.astype(jnp.int32), axis=1)
        place = group * list_len + pos
        hit = places[:, None] == place[None, :]

        def pick(value):
            return jnp.sum(jnp.where(hit, value[None, :], 0), axis=1)

        sub_at = pick(sub + 1)
        before = jnp.concatenate([jnp.zeros((1,), jnp.int32), sub_at[:-1]])
        keep = (sub_at == before) & (places % list_len > 0)
        buckets = jnp.arange(n * n_sub, dtype=jnp.int32)
        in_bucket = buckets[:, None] == (group * n_sub + sub)[None, :]
        last = jnp.max(jnp.where(in_bucket, pos[None, :] + 1, 0), axis=1)
        return pick(slots), pick(row), pick(local_col), keep.astype(jnp.int32), last, place

    by_col = build(col * tile_rows + row, local_col, cols_dev)
    by_row = build(row * tile_cols + col, row, tile_rows)
    return by_col, by_row


def forward_kernel(
    dims, slot_tab, row_tab, keep_tab, last_tab, x_ref, cot_ref, w_ref,
    hidden_ref, grads_ref, xt_ref,
    xg, ww, buf, part, send, recv, cot, load_sem, ag_send, ag_recv, rs_send, rs_recv,
):
    n, tile_rows, cols_dev, list_len, rows, tile, dp_size = dims
    ring = Ring(n)
    half = ring.half
    me = lax.axis_index("tp")
    piece_cols = cols_dev // 2
    piece_rows = tile_rows // 2

    own_rows = pl.ds(pl.multiple_of(me * rows, rows), rows)
    loads = [
        pltpu.make_async_copy(x_ref, xg.at[:, own_rows, :], load_sem.at[0]),
        pltpu.make_async_copy(w_ref.at[0], ww.at[:, :, pl.ds(0, tile)], load_sem.at[1]),
        pltpu.make_async_copy(w_ref.at[1], ww.at[:, :, pl.ds(tile, tile)], load_sem.at[2]),
        pltpu.make_async_copy(cot_ref, cot, load_sem.at[3]),
    ]
    for load in loads:
        load.start()

    barrier = pltpu.get_barrier_semaphore()
    for offset in (1, -1):
        pl.semaphore_signal(
            barrier, inc=1, device_id={"tp": ring.at(offset)}, device_id_type=MESH
        )
    pl.semaphore_wait(barrier, 2)
    loads[0].wait()

    def token_copy(way, piece, hop):
        shard = ring.at(-step_of(way) * hop)
        view = xg.at[
            pl.ds(piece * piece_rows, piece_rows),
            pl.ds(pl.multiple_of(shard * rows, rows), rows),
            :,
        ]
        return pltpu.make_async_remote_copy(
            src_ref=view, dst_ref=view,
            send_sem=ag_send.at[way, piece, hop], recv_sem=ag_recv.at[way, piece, hop],
            device_id={"tp": ring.at(step_of(way))}, device_id_type=MESH,
        )

    lanes = [(way, piece) for piece in range(2) for way in range(2)]
    for way, piece in lanes:
        token_copy(way, piece, 0).start()
    for hop in range(half):
        for way, piece in lanes:
            if hop < hops(ring, way, piece):
                token_copy(way, piece, hop).wait_recv()
                if hop + 1 < hops(ring, way, piece):
                    token_copy(way, piece, hop + 1).start()
    loads[1].wait()
    loads[2].wait()

    buf[0] = jnp.zeros(buf.shape[1:], buf.dtype)

    def compute(which, dest):
        def tile_step(j):
            at = dest * list_len + j
            term = jnp.dot(
                xg[row_tab[at]], ww[slot_tab[at]], preferred_element_type=jnp.float32
            )
            buf[j + 1] = term + jnp.where(keep_tab[at] > 0, buf[j], 0.0)

        unrolled(list_len, tile_step)

        def column(c, carry):
            part[which, c] = buf[last_tab[dest * cols_dev + c]]
            return carry

        lax.fori_loop(0, cols_dev, column, 0)

    def sum_copy(way, piece, hop):
        return pltpu.make_async_remote_copy(
            src_ref=send.at[way, piece, hop], dst_ref=recv.at[way, piece, hop],
            send_sem=rs_send.at[way, piece, hop], recv_sem=rs_recv.at[way, piece, hop],
            device_id={"tp": ring.at(step_of(way))}, device_id_type=MESH,
        )

    def first_hop(way, piece):
        return half - hops(ring, way, piece)

    def push(which, way, piece, hop):
        fresh = hop == first_hop(way, piece)
        if not fresh:
            sum_copy(way, piece, hop - 1).wait_recv()

        def column(c, carry):
            value = part[which, piece * piece_cols + c]
            if not fresh:
                value = value + recv[way, piece, hop - 1, c].astype(jnp.float32)
            send[way, piece, hop, c] = value.astype(jnp.bfloat16)
            return carry

        lax.fori_loop(0, piece_cols, column, 0)
        sum_copy(way, piece, hop).start()

    compute(0, ring.at(half))
    push(0, 0, 0, 0)
    push(0, 1, 1, 0)

    for hop in range(1, half):
        compute(0, ring.at(half - hop))
        compute(1, ring.at(hop - half))
        push(0, 0, 1, hop)
        push(1, 1, 0, hop)
        push(0, 0, 0, hop)
        push(1, 1, 1, hop)

    compute(0, me)

    band = tile // dp_size
    parts = dp_size // CORES
    order = lax.broadcasted_iota(jnp.int32, (tile, tile), 0)
    source = lax.broadcasted_iota(jnp.int32, (tile, tile), 1)
    core = order // (parts * band)
    x_part = order // band % parts
    perm = (source == (x_part * CORES + core) * band + order % band).astype(jnp.bfloat16)

    def transpose_block(r, carry):
        turned = lax.dot_general(
            perm, xg[r], (((1,), (1,)), ((), ())), preferred_element_type=jnp.float32
        ).astype(jnp.bfloat16)
        for c in range(CORES):
            xt_ref[c, r] = turned[c * (tile // CORES) : (c + 1) * (tile // CORES)]
        return carry

    lax.fori_loop(0, tile_rows, transpose_block, 0)
    loads[3].wait()

    for piece in (1, 0):
        for way in range(2):
            sum_copy(way, piece, half - 1).wait_recv()
        for k in range(piece_cols):
            c = piece * piece_cols + k
            total = (
                part[0, c]
                + recv[0, piece, half - 1, k].astype(jnp.float32)
                + recv[1, piece, half - 1, k].astype(jnp.float32)
            )
            gate, up = total[:, :tile], total[:, tile:]
            s = jax.nn.sigmoid(gate)
            act = gate * s
            cotangent = cot[:, c * tile : (c + 1) * tile].astype(jnp.float32)
            hidden_ref[:, c * tile : (c + 1) * tile] = (act * up).astype(jnp.bfloat16)
            grads_ref[c, :, :tile] = (
                cotangent * up * (s * (1.0 + gate * (1.0 - s)))
            ).astype(jnp.bfloat16)
            grads_ref[c, :, tile:] = (cotangent * act).astype(jnp.bfloat16)

    for way, piece in lanes:
        for hop in range(hops(ring, way, piece)):
            token_copy(way, piece, hop).wait_send()
        for hop in range(first_hop(way, piece), half):
            sum_copy(way, piece, hop).wait_send()


def forward(tables, x, cotangent, weights, n, list_len, dp_size):
    slot_tab, row_tab, _, keep_tab, last_tab, _ = tables
    tile_rows, rows, tile = x.shape
    tokens, cols = cotangent.shape
    owned = weights.shape[1]
    cols_dev = cols // tile
    half = n // 2
    dims = (n, tile_rows, cols_dev, list_len, rows, tile, dp_size)
    smem = pl.BlockSpec(memory_space=pltpu.SMEM)
    hbm = pl.BlockSpec(memory_space=pl.ANY)
    vmem = pl.BlockSpec(memory_space=pltpu.VMEM)
    slots = (2, 2, half, cols_dev // 2, tokens, 2 * tile)
    return pl.pallas_call(
        functools.partial(forward_kernel, dims),
        name="forward",
        in_specs=[smem] * 4 + [hbm] * 3,
        out_specs=[vmem, vmem, vmem],
        out_shape=[
            jax.ShapeDtypeStruct((tokens, cols), jnp.bfloat16),
            jax.ShapeDtypeStruct((cols_dev, tokens, 2 * tile), jnp.bfloat16),
            jax.ShapeDtypeStruct((CORES, tile_rows, tile // CORES, tokens), jnp.bfloat16),
        ],
        scratch_shapes=[
            pltpu.VMEM((tile_rows, tokens, tile), jnp.bfloat16),
            pltpu.VMEM((owned, tile, 2 * tile), jnp.bfloat16),
            pltpu.VMEM((list_len + 1, tokens, 2 * tile), jnp.float32),
            pltpu.VMEM((2, cols_dev, tokens, 2 * tile), jnp.float32),
            pltpu.VMEM(slots, jnp.bfloat16),
            pltpu.VMEM(slots, jnp.bfloat16),
            pltpu.VMEM((tokens, cols), jnp.bfloat16),
            pltpu.SemaphoreType.DMA((4,)),
            pltpu.SemaphoreType.DMA((2, 2, half)),
            pltpu.SemaphoreType.DMA((2, 2, half)),
            pltpu.SemaphoreType.DMA((2, 2, half)),
            pltpu.SemaphoreType.DMA((2, 2, half)),
        ],
        compiler_params=pltpu.CompilerParams(
            collective_id=0, has_side_effects=True, vmem_limit_bytes=VMEM_LIMIT
        ),
    )(slot_tab, row_tab, keep_tab, last_tab, x, cotangent, weights)


def backward_kernel(
    dims, big, slot_tab, row_tab, col_tab, keep_tab, last_tab, grads_ref, xt_ref, w_ref,
    d_ref, parts_ref, *rest,
):
    n, tile_rows, cols_dev, list_len, rows, tokens, tile, dp_size = dims
    (gall, gw, ww, xt, buf, dx, stage, send, recv,
     load_sem, work_sem, g_send, g_recv, p_send, p_recv, t_sem,
     x_send, x_recv, x_local, rs_send, rs_recv) = rest
    ring = Ring(n)
    half = ring.half
    me = lax.axis_index("tp")
    me_dp = lax.axis_index("dp")
    core, x_part = lax.rem(me_dp, CORES), lax.div(me_dp, CORES)
    n_parts = dp_size // CORES
    band = tile // dp_size
    piece_cols = cols_dev // 2
    piece_rows = tile_rows // 2
    n_stage = stage.shape[0]
    partner = {"dp": x_part * CORES + 1 - core}

    own_cols = pl.ds(pl.multiple_of(me * cols_dev, cols_dev), cols_dev)
    loads = [
        pltpu.make_async_copy(grads_ref, gall.at[0, own_cols], load_sem.at[0]),
        pltpu.make_async_copy(xt_ref.at[core], xt.at[0], load_sem.at[1]),
        pltpu.make_async_copy(w_ref.at[0], ww.at[:, :, pl.ds(0, tile)], load_sem.at[2]),
        pltpu.make_async_copy(w_ref.at[1], ww.at[:, :, pl.ds(tile, tile)], load_sem.at[3]),
    ]
    for load in loads:
        load.start()

    barrier = pltpu.get_barrier_semaphore()
    for offset in (1, -1):
        pl.semaphore_signal(
            barrier, inc=1, device_id={"tp": ring.at(offset)}, device_id_type=MESH
        )
    pl.semaphore_signal(barrier, inc=1, device_id=partner, device_id_type=MESH)

    def x_device(off):
        return {"dp": lax.rem(x_part + off, n_parts) * CORES + core}

    for off in range(1, n_parts):
        pl.semaphore_signal(barrier, inc=1, device_id=x_device(off), device_id_type=MESH)
    pl.semaphore_wait(barrier, 3 + n_parts - 1)

    turned = pltpu.make_async_remote_copy(
        src_ref=xt_ref.at[1 - core], dst_ref=xt.at[1],
        send_sem=t_sem.at[0], recv_sem=t_sem.at[1],
        device_id=partner, device_id_type=MESH,
    )

    def piece_view(side, shard, piece):
        start = pl.multiple_of(shard * cols_dev + piece * piece_cols, piece_cols)
        return gall.at[side, pl.ds(start, piece_cols)]

    def grad_copy(way, piece, hop):
        view = piece_view(0, ring.at(-step_of(way) * hop), piece)
        return pltpu.make_async_remote_copy(
            src_ref=view, dst_ref=view,
            send_sem=g_send.at[way, piece, hop], recv_sem=g_recv.at[way, piece, hop],
            device_id={"tp": ring.at(step_of(way))}, device_id_type=MESH,
        )

    def group_number(offset):
        return offset % n

    def pair_copy(offset, piece):
        shard = ring.at(offset)
        g = group_number(offset)
        return pltpu.make_async_remote_copy(
            src_ref=piece_view(0, shard, piece), dst_ref=piece_view(1, shard, piece),
            send_sem=p_send.at[g, piece], recv_sem=p_recv.at[g, piece],
            device_id=partner, device_id_type=MESH,
        )

    def x_copy(i, offset, off):
        dest = lax.rem(x_part + off, n_parts)
        shard = ring.at(offset)
        return pltpu.make_async_remote_copy(
            src_ref=stage.at[i % n_stage, dest],
            dst_ref=parts_ref.at[
                x_part, pl.ds(pl.multiple_of(shard * list_len, list_len), list_len)
            ],
            send_sem=x_send.at[i, off - 1], recv_sem=x_recv.at[i, off - 1],
            device_id=x_device(off), device_id_type=MESH,
        )

    def keep_copy(i, offset):
        shard = ring.at(offset)
        return pltpu.make_async_copy(
            stage.at[i % n_stage, x_part],
            parts_ref.at[
                x_part, pl.ds(pl.multiple_of(shard * list_len, list_len), list_len)
            ],
            x_local.at[i],
        )

    def finish(i, offset):
        for off in range(1, n_parts):
            x_copy(i, offset, off).wait_send()
        keep_copy(i, offset).wait()

    lanes = [(0, 0), (1, 1), (0, 1), (1, 0)]
    loads[0].wait()
    for way, piece in lanes:
        grad_copy(way, piece, 0).start()
    for piece in range(2):
        pair_copy(0, piece).start()
    turned.start()

    dx[...] = jnp.zeros(dx.shape, dx.dtype)
    buf[0] = jnp.zeros(buf.shape[1:], buf.dtype)
    loads[1].wait()
    turned.wait()

    done = []
    cells = {}

    def weight_grads(offset, cell):
        i = len(done)
        shard = ring.at(offset)
        for piece in range(2):
            pair_copy(offset, piece).wait_recv()
        cols = pl.ds(pl.multiple_of(shard * cols_dev, cols_dev), cols_dev)
        fills = [
            pltpu.make_async_copy(gall.at[side, cols], gw.at[cell, side], work_sem.at[side])
            for side in range(2)
        ]
        for fill in fills:
            fill.start()
        if i >= n_stage:
            finish(i - n_stage, done[i - n_stage])
        for fill in fills:
            fill.wait()
        slot = i % n_stage

        def outer(j):
            at = shard * list_len + j
            r, c = row_tab[at], col_tab[at]
            value = jnp.dot(
                xt[0, r], gw[cell, 0, c], preferred_element_type=jnp.float32
            ) + jnp.dot(xt[1, r], gw[cell, 1, c], preferred_element_type=jnp.float32)
            for k in range(n_parts):
                stage[slot, k, j] = value[k * band : (k + 1) * band].astype(jnp.bfloat16)

        unrolled(list_len, outer)
        for off in range(1, n_parts):
            x_copy(i, offset, off).start()
        keep_copy(i, offset).start()
        done.append(offset)
        cells[offset] = cell

    def token_grads(offset):
        shard = ring.at(offset)
        cell = cells[offset]

        def back(j):
            at = shard * list_len + j
            term = lax.dot_general(
                gw[cell, 0, col_tab[at]], ww[slot_tab[at]], (((1,), (1,)), ((), ())),
                preferred_element_type=jnp.float32,
            )
            buf[j + 1] = term + jnp.where(keep_tab[at] > 0, buf[j], 0.0)

        unrolled(list_len, back)

        def add_row(r):
            dx[r] += buf[last_tab[shard * tile_rows + r]]

        unrolled(tile_rows, add_row)

    def arrive(way, piece, hop):
        if hop >= hops(ring, way, piece):
            return
        grad_copy(way, piece, hop).wait_recv()
        if hop + 1 < hops(ring, way, piece):
            grad_copy(way, piece, hop + 1).start()
        pair_copy(-step_of(way) * (hop + 1), piece).start()

    weight_grads(0, 0)
    loads[2].wait()
    loads[3].wait()
    token_grads(0)
    for hop in range(half):
        arrive(0, 0, hop)
        arrive(1, 1, hop)
        if hop == half - 1:
            weight_grads(half, 2)
        if hop > 0:
            token_grads(-hop)
            token_grads(hop)
        if hop == half - 1:
            token_grads(half)
        else:
            arrive(0, 1, hop)
            arrive(1, 0, hop)
            weight_grads(-hop - 1, 0)
            weight_grads(hop + 1, 1)

    def sum_copy(way, piece, hop):
        return pltpu.make_async_remote_copy(
            src_ref=send.at[way, piece, hop], dst_ref=recv.at[way, piece, hop],
            send_sem=rs_send.at[way, piece, hop], recv_sem=rs_recv.at[way, piece, hop],
            device_id={"tp": ring.at(step_of(way))}, device_id_type=MESH,
        )

    def first_hop(way, piece):
        return half - hops(ring, way, piece)

    def own_term(dest, piece):
        return dx[
            pl.ds(piece * piece_rows, piece_rows),
            pl.ds(pl.multiple_of(dest * rows, rows), rows),
            :,
        ]

    def push(way, piece, hop):
        value = own_term(ring.at(step_of(way) * (half - hop)), piece)
        if hop > first_hop(way, piece):
            sum_copy(way, piece, hop - 1).wait_recv()
            value = value + recv[way, piece, hop - 1].astype(jnp.float32)
        send[way, piece, hop] = value.astype(jnp.bfloat16)
        sum_copy(way, piece, hop).start()

    push(0, 0, 0)
    push(1, 1, 0)
    for hop in range(1, half):
        for way, piece in ((0, 1), (1, 0), (0, 0), (1, 1)):
            push(way, piece, hop)
    for piece in range(2):
        for way in range(2):
            sum_copy(way, piece, half - 1).wait_recv()
        d_ref[pl.ds(piece * piece_rows, piece_rows)] = (
            own_term(me, piece)
            + recv[0, piece, half - 1].astype(jnp.float32)
            + recv[1, piece, half - 1].astype(jnp.float32)
        ).astype(jnp.bfloat16)

    for i in range(max(0, n - n_stage), n):
        finish(i, done[i])
    for i in range(n):
        for off in range(1, n_parts):
            x_copy(i, done[i], off).wait_recv()
    for way, piece in lanes:
        for hop in range(hops(ring, way, piece)):
            grad_copy(way, piece, hop).wait_send()
        for hop in range(first_hop(way, piece), half):
            sum_copy(way, piece, hop).wait_send()
    for offset in done:
        for piece in range(2):
            pair_copy(offset, piece).wait_send()


def backward(tables, grads, xt, weights, n, list_len, rows, dp_size):
    slot_tab, row_tab, col_tab, keep_tab, last_tab, _ = tables
    _, tile_rows, half_tile, tokens = xt.shape
    cols_dev, _, pair = grads.shape
    tile = pair // 2
    owned = weights.shape[1]
    half = n // 2
    band = tile // dp_size
    n_parts = dp_size // CORES
    n_stage = 4
    dims = (n, tile_rows, cols_dev, list_len, rows, tokens, tile, dp_size)
    smem = pl.BlockSpec(memory_space=pltpu.SMEM)
    hbm = pl.BlockSpec(memory_space=pl.ANY)
    vmem = pl.BlockSpec(memory_space=pltpu.VMEM)
    slots = (2, 2, half, tile_rows // 2, rows, tile)
    gall_shape = (2, n * cols_dev, tokens, pair)
    big = 2 * n * cols_dev * tokens * pair * 2 > 24 * 2**20
    sem = pltpu.SemaphoreType.DMA
    out_specs = [vmem, hbm]
    out_shape = [
        jax.ShapeDtypeStruct((tile_rows, rows, tile), jnp.bfloat16),
        jax.ShapeDtypeStruct((n_parts, n * list_len, band, pair), jnp.bfloat16),
    ]
    scratch = []
    if big:
        out_specs.append(hbm)
        out_shape.append(jax.ShapeDtypeStruct(gall_shape, jnp.bfloat16))
    else:
        scratch.append(pltpu.VMEM(gall_shape, jnp.bfloat16))
    scratch += [
        pltpu.VMEM((3, 2, cols_dev, tokens, pair), jnp.bfloat16),
        pltpu.VMEM((owned, tile, pair), jnp.bfloat16),
        pltpu.VMEM((2, tile_rows, half_tile, tokens), jnp.bfloat16),
        pltpu.VMEM((list_len + 1, tokens, tile), jnp.float32),
        pltpu.VMEM((tile_rows, tokens, tile), jnp.float32),
        pltpu.VMEM((n_stage, n_parts, list_len, band, pair), jnp.bfloat16),
        pltpu.VMEM(slots, jnp.bfloat16),
        pltpu.VMEM(slots, jnp.bfloat16),
        sem((4,)), sem((2,)),
        sem((2, 2, half)), sem((2, 2, half)),
        sem((n, 2)), sem((n, 2)), sem((2,)),
        sem((n, n_parts - 1)), sem((n, n_parts - 1)), sem((n,)),
        sem((2, 2, half)), sem((2, 2, half)),
    ]
    results = pl.pallas_call(
        functools.partial(backward_kernel, dims, big),
        name="backward",
        in_specs=[smem] * 5 + [hbm] * 3,
        out_specs=out_specs,
        out_shape=out_shape,
        scratch_shapes=scratch,
        compiler_params=pltpu.CompilerParams(
            collective_id=1, has_side_effects=True, vmem_limit_bytes=VMEM_LIMIT
        ),
    )(slot_tab, row_tab, col_tab, keep_tab, last_tab, grads, xt, weights)
    return results[0], results[1]


def finish_kernel(place_ref, parts_ref, out_ref):
    n_parts = parts_ref.shape[0]
    _, chunk, _, tile = out_ref.shape
    base = pl.program_id(0) * chunk

    def one(p, carry):
        at = place_ref[base + p]
        total = parts_ref[0, at].astype(jnp.float32)
        for k in range(1, n_parts):
            total = total + parts_ref[k, at].astype(jnp.float32)
        out_ref[0, p] = total[:, :tile]
        out_ref[1, p] = total[:, tile:]
        return carry

    lax.fori_loop(0, chunk, one, 0)


def finish_sum(place, parts):
    owned = place.shape[0]
    n_parts, listed, band, pair = parts.shape
    tile = pair // 2
    steps = 8
    return pl.pallas_call(
        finish_kernel,
        name="finish",
        grid=(steps,),
        in_specs=[
            pl.BlockSpec(memory_space=pltpu.SMEM),
            pl.BlockSpec((n_parts, listed, band, pair), lambda i: (0, 0, 0, 0)),
        ],
        out_specs=pl.BlockSpec((2, owned // steps, band, tile), lambda i: (0, i, 0, 0)),
        out_shape=jax.ShapeDtypeStruct((2, owned, band, tile), jnp.float32),
        compiler_params=pltpu.CompilerParams(vmem_limit_bytes=VMEM_LIMIT),
    )(place, parts)


def local(normed, cotangent, weight_tiles, slot_tile):
    n = lax.axis_size("tp")
    dp_size = lax.axis_size("dp")
    me = lax.axis_index("tp")
    rows, width = normed.shape
    owned, tile = weight_tiles.shape[1:3]
    tile_rows = width // tile
    tile_cols = cotangent.shape[1] // tile * n
    base_count = owned // n
    list_len = base_count + base_count // 4
    by_col, by_row = build_tables(slot_tile, me, owned, tile_rows, tile_cols, n, list_len)
    x = normed.reshape(rows, tile_rows, tile).transpose(1, 0, 2)
    hidden, grads, xt = forward(by_col, x, cotangent, weight_tiles, n, list_len, dp_size)
    d, parts = backward(by_row, grads, xt, weight_tiles, n, list_len, rows, dp_size)
    grad_tiles = finish_sum(by_row[-1], parts)
    d_normed = d.transpose(1, 0, 2).reshape(rows, width)
    return hidden, d_normed, grad_tiles


def solution(mesh):
    return jax.shard_map(
        local,
        mesh=mesh,
        in_specs=(P(("dp", "tp"), None), P("dp", "tp"), P(None, "tp", None, None), P()),
        out_specs=(P("dp", "tp"), P(("dp", "tp"), None), P(None, "tp", "dp", None)),
        check_vma=False,
    )
```

```python
import functools

import jax
import jax.numpy as jnp
from jax import lax
from jax.experimental import pallas as pl
from jax.experimental.pallas import tpu as pltpu
from jax.sharding import PartitionSpec as P

MESH = pl.DeviceIdType.MESH
VMEM_LIMIT = 67_043_328
CORES = 2


def ring_width(n):
    width = 2
    while 4 * width * width <= n:
        width *= 2
    return width


def ring_pos(index, n):
    y_size = ring_width(n)
    z, y = index // y_size, index % y_size
    inner = (y + y_size - 1) // y_size
    odd = z % 2
    snake = z * (y_size - 1) + (1 - odd) * (y - 1) + odd * (y_size - 1 - y)
    return inner * snake + (1 - inner) * (n - 1 - z)


def ring_index(pos, n):
    y_size = ring_width(n)
    z_size = n // y_size
    back = lax.div(pos, n - z_size)
    z = lax.div(pos, y_size - 1)
    k = lax.rem(pos, y_size - 1)
    odd = lax.rem(z, 2)
    y = (1 - odd) * (k + 1) + odd * (y_size - 1 - k)
    return (1 - back) * (z * y_size + y) + back * (n - 1 - pos) * y_size


def arrival(index, me, n):
    offset = (ring_pos(index, n) - ring_pos(me, n) + n) % n
    behind = 2 * (n - offset) - 1
    return jnp.where(offset == 0, 0, jnp.where(offset < n // 2, 2 * offset, behind))


def arrival_plan(n, owned):
    base = owned // n
    low, high = base - base // 4, base + base // 4
    chunks, cells, start = [], 4, 0
    for step in range(n // 2 + 1):
        landed = min(2 * step + 1, n)
        stop = max(low * landed, owned - high * (n - landed))
        cells = max(cells, landed - start // high)
        if stop - start > high:
            middle = start + (stop - start) // 4 * 2
            chunks += [(step, start, middle - start), (step, middle, stop - middle)]
        else:
            chunks.append((step, start, stop - start))
        start = stop
    return chunks, cells


class Ring:
    def __init__(self, n):
        self.n = n
        self.half = n // 2
        self.pos = ring_pos(lax.axis_index("tp"), n)

    def at(self, offset):
        return ring_index(lax.rem(self.pos + offset + self.n, self.n), self.n)


def hops(ring, way, piece):
    return ring.half if way == piece else ring.half - 1


def step_of(way):
    return 1 - 2 * way


def unrolled(count, body):
    by = 4 if count % 4 == 0 else 2 if count % 2 == 0 else 1

    def steps(i, carry):
        for u in range(by):
            body(i * by + u)
        return carry

    lax.fori_loop(0, count // by, steps, 0)


def build_tables(slot_tile, me, owned, tile_rows, tile_cols, n, list_len):
    cols_dev = tile_cols // n
    mine = lax.dynamic_slice(slot_tile, (me * owned,), (owned,))
    row, col = mine // tile_cols, mine % tile_cols
    group = col // cols_dev
    local_col = col % cols_dev
    same = group[None, :] == group[:, None]
    places = jnp.arange(n * list_len, dtype=jnp.int32)
    slots = jnp.arange(owned, dtype=jnp.int32)

    def build(key, sub, n_sub):
        less = same & (key[None, :] < key[:, None])
        pos = jnp.sum(less.astype(jnp.int32), axis=1)
        place = group * list_len + pos
        hit = places[:, None] == place[None, :]

        def pick(value):
            return jnp.sum(jnp.where(hit, value[None, :], 0), axis=1)

        sub_at = pick(sub + 1)
        before = jnp.concatenate([jnp.zeros((1,), jnp.int32), sub_at[:-1]])
        keep = (sub_at == before) & (places % list_len > 0)
        buckets = jnp.arange(n * n_sub, dtype=jnp.int32)
        in_bucket = buckets[:, None] == (group * n_sub + sub)[None, :]
        last = jnp.max(jnp.where(in_bucket, pos[None, :] + 1, 0), axis=1)
        return pick(slots), pick(row), pick(local_col), keep.astype(jnp.int32), last, place

    by_col = build(col * tile_rows + row, local_col, cols_dev)
    by_row = build(row * tile_cols + col, row, tile_rows)

    order = arrival(group, me, n)
    key = order * owned + slots
    rank = jnp.sum((key[None, :] < key[:, None]).astype(jnp.int32), axis=1)
    _, cells = arrival_plan(n, owned)
    block = order % cells * cols_dev + local_col
    hit = slots[:, None] == rank[None, :]

    def pick(value):
        return jnp.sum(jnp.where(hit, value[None, :], 0), axis=1)

    return by_col, by_row, (pick(row), pick(block), rank)


def forward_kernel(
    dims, slot_tab, row_tab, keep_tab, last_tab, x_ref, cot_ref, w_ref,
    hidden_ref, grads_ref, xt_ref,
    xg, ww, buf, part, send, recv, cot, x_sem, load_sem, ag_send, ag_recv, rs_send, rs_recv,
):
    n, tile_rows, cols_dev, list_len, rows, tile, dp_size = dims
    ring = Ring(n)
    half = ring.half
    me = lax.axis_index("tp")
    piece_cols = cols_dev // 2
    piece_rows = tile_rows // 2

    own_rows = pl.ds(pl.multiple_of(me * rows, rows), rows)
    loads = [
        pltpu.make_async_copy(cot_ref, cot, load_sem.at[3]),
        pltpu.make_async_copy(w_ref.at[0], ww.at[:, :, pl.ds(0, tile)], load_sem.at[1]),
        pltpu.make_async_copy(w_ref.at[1], ww.at[:, :, pl.ds(tile, tile)], load_sem.at[2]),
    ]
    own = [
        pltpu.make_async_copy(
            x_ref.at[:, pl.ds(r * tile, tile)], xg.at[r, own_rows, :], x_sem.at[r]
        )
        for r in range(tile_rows)
    ]
    for load in own + loads:
        load.start()

    barrier = pltpu.get_barrier_semaphore()
    for offset in (1, -1):
        pl.semaphore_signal(
            barrier, inc=1, device_id={"tp": ring.at(offset)}, device_id_type=MESH
        )
    pl.semaphore_wait(barrier, 2)
    for load in own:
        load.wait()

    def token_copy(way, piece, hop):
        shard = ring.at(-step_of(way) * hop)
        view = xg.at[
            pl.ds(piece * piece_rows, piece_rows),
            pl.ds(pl.multiple_of(shard * rows, rows), rows),
            :,
        ]
        return pltpu.make_async_remote_copy(
            src_ref=view, dst_ref=view,
            send_sem=ag_send.at[way, piece, hop], recv_sem=ag_recv.at[way, piece, hop],
            device_id={"tp": ring.at(step_of(way))}, device_id_type=MESH,
        )

    lanes = [(way, piece) for piece in range(2) for way in range(2)]
    for way, piece in lanes:
        token_copy(way, piece, 0).start()
    for hop in range(half):
        for way, piece in lanes:
            if hop < hops(ring, way, piece):
                token_copy(way, piece, hop).wait_recv()
                if hop + 1 < hops(ring, way, piece):
                    token_copy(way, piece, hop + 1).start()
    loads[1].wait()
    loads[2].wait()

    buf[0] = jnp.zeros(buf.shape[1:], buf.dtype)

    def compute(which, dest):
        def tile_step(j):
            at = dest * list_len + j
            term = jnp.dot(
                xg[row_tab[at]], ww[slot_tab[at]], preferred_element_type=jnp.float32
            )
            buf[j + 1] = term + jnp.where(keep_tab[at] > 0, buf[j], 0.0)

        unrolled(list_len, tile_step)

        def column(c, carry):
            part[which, c] = buf[last_tab[dest * cols_dev + c]]
            return carry

        lax.fori_loop(0, cols_dev, column, 0)

    def sum_copy(way, piece, hop):
        return pltpu.make_async_remote_copy(
            src_ref=send.at[way, piece, hop], dst_ref=recv.at[way, piece, hop],
            send_sem=rs_send.at[way, piece, hop], recv_sem=rs_recv.at[way, piece, hop],
            device_id={"tp": ring.at(step_of(way))}, device_id_type=MESH,
        )

    def first_hop(way, piece):
        return half - hops(ring, way, piece)

    def push(which, way, piece, hop):
        fresh = hop == first_hop(way, piece)
        if not fresh:
            sum_copy(way, piece, hop - 1).wait_recv()

        def column(c, carry):
            value = part[which, piece * piece_cols + c]
            if not fresh:
                value = value + recv[way, piece, hop - 1, c].astype(jnp.float32)
            send[way, piece, hop, c] = value.astype(jnp.bfloat16)
            return carry

        lax.fori_loop(0, piece_cols, column, 0)
        sum_copy(way, piece, hop).start()

    compute(0, ring.at(half))
    push(0, 0, 0, 0)
    push(0, 1, 1, 0)

    for hop in range(1, half):
        compute(0, ring.at(half - hop))
        compute(1, ring.at(hop - half))
        push(0, 0, 1, hop)
        push(1, 1, 0, hop)
        push(0, 0, 0, hop)
        push(1, 1, 1, hop)

    compute(0, me)

    band = tile // dp_size
    parts = dp_size // CORES
    order = lax.broadcasted_iota(jnp.int32, (tile, tile), 0)
    source = lax.broadcasted_iota(jnp.int32, (tile, tile), 1)
    core = order // (parts * band)
    x_part = order // band % parts
    perm = (source == (x_part * CORES + core) * band + order % band).astype(jnp.bfloat16)

    def transpose_block(r, carry):
        turned = lax.dot_general(
            perm, xg[r], (((1,), (1,)), ((), ())), preferred_element_type=jnp.float32
        ).astype(jnp.bfloat16)
        for c in range(CORES):
            xt_ref[c, r] = turned[c * (tile // CORES) : (c + 1) * (tile // CORES)]
        return carry

    lax.fori_loop(0, tile_rows, transpose_block, 0)
    loads[0].wait()

    for piece in (1, 0):
        for way in range(2):
            sum_copy(way, piece, half - 1).wait_recv()
        for k in range(piece_cols):
            c = piece * piece_cols + k
            total = (
                part[0, c]
                + recv[0, piece, half - 1, k].astype(jnp.float32)
                + recv[1, piece, half - 1, k].astype(jnp.float32)
            )
            gate, up = total[:, :tile], total[:, tile:]
            s = jax.nn.sigmoid(gate)
            act = gate * s
            cotangent = cot[:, c * tile : (c + 1) * tile].astype(jnp.float32)
            hidden_ref[:, c * tile : (c + 1) * tile] = (act * up).astype(jnp.bfloat16)
            grads_ref[c, :, :tile] = (
                cotangent * up * (s * (1.0 + gate * (1.0 - s)))
            ).astype(jnp.bfloat16)
            grads_ref[c, :, tile:] = (cotangent * act).astype(jnp.bfloat16)

    for way, piece in lanes:
        for hop in range(hops(ring, way, piece)):
            token_copy(way, piece, hop).wait_send()
        for hop in range(first_hop(way, piece), half):
            sum_copy(way, piece, hop).wait_send()


def forward(tables, x, cotangent, weights, n, list_len, dp_size):
    slot_tab, row_tab, _, keep_tab, last_tab, _ = tables
    rows, width = x.shape
    tile = weights.shape[2]
    tile_rows = width // tile
    tokens, cols = cotangent.shape
    owned = weights.shape[1]
    cols_dev = cols // tile
    half = n // 2
    dims = (n, tile_rows, cols_dev, list_len, rows, tile, dp_size)
    smem = pl.BlockSpec(memory_space=pltpu.SMEM)
    hbm = pl.BlockSpec(memory_space=pl.ANY)
    vmem = pl.BlockSpec(memory_space=pltpu.VMEM)
    slots = (2, 2, half, cols_dev // 2, tokens, 2 * tile)
    return pl.pallas_call(
        functools.partial(forward_kernel, dims),
        name="forward",
        in_specs=[smem] * 4 + [hbm] * 3,
        out_specs=[vmem, vmem, vmem],
        out_shape=[
            jax.ShapeDtypeStruct((tokens, cols), jnp.bfloat16),
            jax.ShapeDtypeStruct((cols_dev, tokens, 2 * tile), jnp.bfloat16),
            jax.ShapeDtypeStruct((CORES, tile_rows, tile // CORES, tokens), jnp.bfloat16),
        ],
        scratch_shapes=[
            pltpu.VMEM((tile_rows, tokens, tile), jnp.bfloat16),
            pltpu.VMEM((owned, tile, 2 * tile), jnp.bfloat16),
            pltpu.VMEM((list_len + 1, tokens, 2 * tile), jnp.float32),
            pltpu.VMEM((2, cols_dev, tokens, 2 * tile), jnp.float32),
            pltpu.VMEM(slots, jnp.bfloat16),
            pltpu.VMEM(slots, jnp.bfloat16),
            pltpu.VMEM((tokens, cols), jnp.bfloat16),
            pltpu.SemaphoreType.DMA((tile_rows,)),
            pltpu.SemaphoreType.DMA((4,)),
            pltpu.SemaphoreType.DMA((2, 2, half)),
            pltpu.SemaphoreType.DMA((2, 2, half)),
            pltpu.SemaphoreType.DMA((2, 2, half)),
            pltpu.SemaphoreType.DMA((2, 2, half)),
        ],
        compiler_params=pltpu.CompilerParams(
            collective_id=0, has_side_effects=True, vmem_limit_bytes=VMEM_LIMIT
        ),
    )(slot_tab, row_tab, keep_tab, last_tab, x, cotangent, weights)


def backward_kernel(
    dims, plan, slot_tab, col_tab, keep_tab, last_tab, list_row, list_block, grads_ref, xt_ref, w_ref,
    d_ref, parts_ref, *rest,
):
    n, tile_rows, cols_dev, list_len, rows, tokens, tile, dp_size = dims
    (gall, gw, ww, xt, buf, dx, stage, send, recv,
     load_sem, work_sem, g_send, g_recv, p_send, p_recv, t_sem,
     x_send, x_recv, x_local, rs_send, rs_recv) = rest
    ring = Ring(n)
    half = ring.half
    me = lax.axis_index("tp")
    me_dp = lax.axis_index("dp")
    core, x_part = lax.rem(me_dp, CORES), lax.div(me_dp, CORES)
    n_parts = dp_size // CORES
    band = tile // dp_size
    piece_cols = cols_dev // 2
    piece_rows = tile_rows // 2
    n_stage = stage.shape[0]
    chunks, cells = plan
    partner = {"dp": x_part * CORES + 1 - core}

    own_cols = pl.ds(pl.multiple_of(me * cols_dev, cols_dev), cols_dev)
    loads = [
        pltpu.make_async_copy(grads_ref, gall.at[0, own_cols], load_sem.at[0]),
        pltpu.make_async_copy(xt_ref.at[core], xt.at[0], load_sem.at[1]),
        pltpu.make_async_copy(w_ref.at[0], ww.at[:, :, pl.ds(0, tile)], load_sem.at[2]),
        pltpu.make_async_copy(w_ref.at[1], ww.at[:, :, pl.ds(tile, tile)], load_sem.at[3]),
    ]
    for load in loads:
        load.start()

    barrier = pltpu.get_barrier_semaphore()
    for offset in (1, -1):
        pl.semaphore_signal(
            barrier, inc=1, device_id={"tp": ring.at(offset)}, device_id_type=MESH
        )
    pl.semaphore_signal(barrier, inc=1, device_id=partner, device_id_type=MESH)

    def x_device(off):
        return {"dp": lax.rem(x_part + off, n_parts) * CORES + core}

    for off in range(1, n_parts):
        pl.semaphore_signal(barrier, inc=1, device_id=x_device(off), device_id_type=MESH)
    pl.semaphore_wait(barrier, 3 + n_parts - 1)

    turned = pltpu.make_async_remote_copy(
        src_ref=xt_ref.at[1 - core], dst_ref=xt.at[1],
        send_sem=t_sem.at[0], recv_sem=t_sem.at[1],
        device_id=partner, device_id_type=MESH,
    )

    def piece_view(side, shard, piece):
        start = pl.multiple_of(shard * cols_dev + piece * piece_cols, piece_cols)
        return gall.at[side, pl.ds(start, piece_cols)]

    def grad_copy(way, piece, hop):
        view = piece_view(0, ring.at(-step_of(way) * hop), piece)
        return pltpu.make_async_remote_copy(
            src_ref=view, dst_ref=view,
            send_sem=g_send.at[way, piece, hop], recv_sem=g_recv.at[way, piece, hop],
            device_id={"tp": ring.at(step_of(way))}, device_id_type=MESH,
        )

    def group_number(offset):
        return offset % n

    def pair_copy(offset, piece):
        shard = ring.at(offset)
        g = group_number(offset)
        return pltpu.make_async_remote_copy(
            src_ref=piece_view(0, shard, piece), dst_ref=piece_view(1, shard, piece),
            send_sem=p_send.at[g, piece], recv_sem=p_recv.at[g, piece],
            device_id=partner, device_id_type=MESH,
        )

    def x_copy(i, off):
        _, start, size = chunks[i]
        dest = lax.rem(x_part + off, n_parts)
        return pltpu.make_async_remote_copy(
            src_ref=stage.at[i % n_stage, dest, pl.ds(0, size)],
            dst_ref=parts_ref.at[x_part, pl.ds(start, size)],
            send_sem=x_send.at[i, off - 1], recv_sem=x_recv.at[i, off - 1],
            device_id=x_device(off), device_id_type=MESH,
        )

    def keep_copy(i):
        _, start, size = chunks[i]
        return pltpu.make_async_copy(
            stage.at[i % n_stage, x_part, pl.ds(0, size)],
            parts_ref.at[x_part, pl.ds(start, size)],
            x_local.at[i],
        )

    def finish(i):
        for off in range(1, n_parts):
            x_copy(i, off).wait_send()
        keep_copy(i).wait()

    lanes = [(0, 0), (1, 1), (0, 1), (1, 0)]
    loads[0].wait()
    for way, piece in lanes:
        grad_copy(way, piece, 0).start()
    for piece in range(2):
        pair_copy(0, piece).start()
    turned.start()

    dx[...] = jnp.zeros(dx.shape, dx.dtype)
    buf[0] = jnp.zeros(buf.shape[1:], buf.dtype)
    loads[1].wait()
    turned.wait()

    offsets = [0]
    for hop in range(1, half):
        offsets += [-hop, hop]
    offsets.append(half)

    def cell_of(offset):
        return offsets.index(offset) % cells * cols_dev

    def weight_grads(step):
        landed = [offset for offset in offsets if abs(offset) == step]
        fills = []
        for number, offset in enumerate(landed):
            for piece in range(2):
                pair_copy(offset, piece).wait_recv()
            cols = pl.ds(pl.multiple_of(ring.at(offset) * cols_dev, cols_dev), cols_dev)
            fills += [
                pltpu.make_async_copy(
                    gall.at[side, cols],
                    gw.at[side, pl.ds(cell_of(offset), cols_dev)],
                    work_sem.at[number, side],
                )
                for side in range(2)
            ]
        for fill in fills:
            fill.start()
        for fill in fills:
            fill.wait()
        for i, (at_step, start, size) in enumerate(chunks):
            if at_step != step:
                continue
            if i >= n_stage:
                finish(i - n_stage)
            slot = i % n_stage

            def outer(j):
                r, block = list_row[start + j], list_block[start + j]
                value = jnp.dot(
                    xt[0, r], gw[0, block], preferred_element_type=jnp.float32
                ) + jnp.dot(xt[1, r], gw[1, block], preferred_element_type=jnp.float32)
                for k in range(n_parts):
                    stage[slot, k, j] = value[k * band : (k + 1) * band].astype(jnp.bfloat16)

            unrolled(size, outer)
            for off in range(1, n_parts):
                x_copy(i, off).start()
            keep_copy(i).start()

    def token_grads(offset):
        shard = ring.at(offset)
        cell = cell_of(offset)

        def back(j):
            at = shard * list_len + j
            term = lax.dot_general(
                gw[0, cell + col_tab[at]], ww[slot_tab[at]], (((1,), (1,)), ((), ())),
                preferred_element_type=jnp.float32,
            )
            buf[j + 1] = term + jnp.where(keep_tab[at] > 0, buf[j], 0.0)

        unrolled(list_len, back)

        def add_row(r):
            dx[r] += buf[last_tab[shard * tile_rows + r]]

        unrolled(tile_rows, add_row)

    def arrive(way, piece, hop):
        if hop >= hops(ring, way, piece):
            return
        grad_copy(way, piece, hop).wait_recv()
        if hop + 1 < hops(ring, way, piece):
            grad_copy(way, piece, hop + 1).start()
        pair_copy(-step_of(way) * (hop + 1), piece).start()

    weight_grads(0)
    loads[2].wait()
    loads[3].wait()
    token_grads(0)
    for hop in range(half):
        arrive(0, 0, hop)
        arrive(1, 1, hop)
        if hop == half - 1:
            weight_grads(half)
        if hop > 0:
            token_grads(-hop)
            token_grads(hop)
        if hop == half - 1:
            token_grads(half)
        else:
            arrive(0, 1, hop)
            arrive(1, 0, hop)
            weight_grads(hop + 1)

    def sum_copy(way, piece, hop):
        return pltpu.make_async_remote_copy(
            src_ref=send.at[way, piece, hop], dst_ref=recv.at[way, piece, hop],
            send_sem=rs_send.at[way, piece, hop], recv_sem=rs_recv.at[way, piece, hop],
            device_id={"tp": ring.at(step_of(way))}, device_id_type=MESH,
        )

    def first_hop(way, piece):
        return half - hops(ring, way, piece)

    def own_term(dest, piece):
        return dx[
            pl.ds(piece * piece_rows, piece_rows),
            pl.ds(pl.multiple_of(dest * rows, rows), rows),
            :,
        ]

    def push(way, piece, hop):
        value = own_term(ring.at(step_of(way) * (half - hop)), piece)
        if hop > first_hop(way, piece):
            sum_copy(way, piece, hop - 1).wait_recv()
            value = value + recv[way, piece, hop - 1].astype(jnp.float32)
        send[way, piece, hop] = value.astype(jnp.bfloat16)
        sum_copy(way, piece, hop).start()

    push(0, 0, 0)
    push(1, 1, 0)
    for hop in range(1, half):
        for way, piece in ((0, 1), (1, 0), (0, 0), (1, 1)):
            push(way, piece, hop)
    for piece in range(2):
        for way in range(2):
            sum_copy(way, piece, half - 1).wait_recv()
        d_ref[pl.ds(piece * piece_rows, piece_rows)] = (
            own_term(me, piece)
            + recv[0, piece, half - 1].astype(jnp.float32)
            + recv[1, piece, half - 1].astype(jnp.float32)
        ).astype(jnp.bfloat16)

    for i in range(max(0, len(chunks) - n_stage), len(chunks)):
        finish(i)
    for i in range(len(chunks)):
        for off in range(1, n_parts):
            x_copy(i, off).wait_recv()
    for way, piece in lanes:
        for hop in range(hops(ring, way, piece)):
            grad_copy(way, piece, hop).wait_send()
        for hop in range(first_hop(way, piece), half):
            sum_copy(way, piece, hop).wait_send()
    for offset in offsets:
        for piece in range(2):
            pair_copy(offset, piece).wait_send()


def backward(tables, listed, grads, xt, weights, n, list_len, rows, dp_size):
    slot_tab, _, col_tab, keep_tab, last_tab, _ = tables
    list_row, list_block, _ = listed
    _, tile_rows, half_tile, tokens = xt.shape
    cols_dev, _, pair = grads.shape
    tile = pair // 2
    owned = weights.shape[1]
    half = n // 2
    band = tile // dp_size
    n_parts = dp_size // CORES
    n_stage = 4
    chunks, cells = plan = arrival_plan(n, owned)
    largest = max(size for _, _, size in chunks)
    dims = (n, tile_rows, cols_dev, list_len, rows, tokens, tile, dp_size)
    smem = pl.BlockSpec(memory_space=pltpu.SMEM)
    hbm = pl.BlockSpec(memory_space=pl.ANY)
    vmem = pl.BlockSpec(memory_space=pltpu.VMEM)
    slots = (2, 2, half, tile_rows // 2, rows, tile)
    gall_shape = (2, n * cols_dev, tokens, pair)
    big = 2 * n * cols_dev * tokens * pair * 2 > 24 * 2**20
    sem = pltpu.SemaphoreType.DMA
    out_specs = [vmem, hbm]
    out_shape = [
        jax.ShapeDtypeStruct((tile_rows, rows, tile), jnp.bfloat16),
        jax.ShapeDtypeStruct((n_parts, owned, band, pair), jnp.bfloat16),
    ]
    scratch = []
    if big:
        out_specs.append(hbm)
        out_shape.append(jax.ShapeDtypeStruct(gall_shape, jnp.bfloat16))
    else:
        scratch.append(pltpu.VMEM(gall_shape, jnp.bfloat16))
    scratch += [
        pltpu.VMEM((2, cells * cols_dev, tokens, pair), jnp.bfloat16),
        pltpu.VMEM((owned, tile, pair), jnp.bfloat16),
        pltpu.VMEM((2, tile_rows, half_tile, tokens), jnp.bfloat16),
        pltpu.VMEM((list_len + 1, tokens, tile), jnp.float32),
        pltpu.VMEM((tile_rows, tokens, tile), jnp.float32),
        pltpu.VMEM((n_stage, n_parts, largest, band, pair), jnp.bfloat16),
        pltpu.VMEM(slots, jnp.bfloat16),
        pltpu.VMEM(slots, jnp.bfloat16),
        sem((4,)), sem((2, 2)),
        sem((2, 2, half)), sem((2, 2, half)),
        sem((n, 2)), sem((n, 2)), sem((2,)),
        sem((len(chunks), n_parts - 1)), sem((len(chunks), n_parts - 1)), sem((len(chunks),)),
        sem((2, 2, half)), sem((2, 2, half)),
    ]
    results = pl.pallas_call(
        functools.partial(backward_kernel, dims, plan),
        name="backward",
        in_specs=[smem] * 6 + [hbm] * 3,
        out_specs=out_specs,
        out_shape=out_shape,
        scratch_shapes=scratch,
        compiler_params=pltpu.CompilerParams(
            collective_id=1, has_side_effects=True, vmem_limit_bytes=VMEM_LIMIT
        ),
    )(slot_tab, col_tab, keep_tab, last_tab, list_row, list_block, grads, xt, weights)
    return results[0], results[1]


def finish_kernel(place_ref, parts_ref, d_ref, hidden_ref, out_ref, d_out, hidden_out):
    n_parts = parts_ref.shape[0]
    _, chunk, _, tile = out_ref.shape
    base = pl.program_id(0) * chunk

    @pl.when(pl.program_id(0) == 0)
    def _():
        for r in range(d_ref.shape[0]):
            d_out[:, r * tile : (r + 1) * tile] = d_ref[r]

    hidden_out[...] = hidden_ref[...]

    def one(p):
        at = place_ref[base + p]
        total = parts_ref[0, at].astype(jnp.float32)
        for k in range(1, n_parts):
            total = total + parts_ref[k, at].astype(jnp.float32)
        out_ref[0, p] = total[:, :tile]
        out_ref[1, p] = total[:, tile:]

    unrolled(chunk, one)


def finish_sum(place, parts, d, hidden):
    owned = place.shape[0]
    n_parts, listed, band, pair = parts.shape
    tile = pair // 2
    tile_rows, rows, _ = d.shape
    tokens, cols = hidden.shape
    steps = 8
    return pl.pallas_call(
        finish_kernel,
        name="finish",
        grid=(steps,),
        in_specs=[
            pl.BlockSpec(memory_space=pltpu.SMEM),
            pl.BlockSpec((n_parts, listed, band, pair), lambda i: (0, 0, 0, 0)),
            pl.BlockSpec((tile_rows, rows, tile), lambda i: (0, 0, 0)),
            pl.BlockSpec((tokens // steps, cols), lambda i: (i, 0)),
        ],
        out_specs=[
            pl.BlockSpec((2, owned // steps, band, tile), lambda i: (0, i, 0, 0)),
            pl.BlockSpec((rows, tile_rows * tile), lambda i: (0, 0)),
            pl.BlockSpec((tokens // steps, cols), lambda i: (i, 0)),
        ],
        out_shape=[
            jax.ShapeDtypeStruct((2, owned, band, tile), jnp.float32),
            jax.ShapeDtypeStruct((rows, tile_rows * tile), d.dtype),
            jax.ShapeDtypeStruct(hidden.shape, hidden.dtype),
        ],
        compiler_params=pltpu.CompilerParams(vmem_limit_bytes=VMEM_LIMIT),
    )(place, parts, d, hidden)


def local(normed, cotangent, weight_tiles, slot_tile):
    n = lax.axis_size("tp")
    dp_size = lax.axis_size("dp")
    me = lax.axis_index("tp")
    rows, width = normed.shape
    owned, tile = weight_tiles.shape[1:3]
    tile_rows = width // tile
    tile_cols = cotangent.shape[1] // tile * n
    base_count = owned // n
    list_len = base_count + base_count // 4
    by_col, by_row, listed = build_tables(
        slot_tile, me, owned, tile_rows, tile_cols, n, list_len
    )
    hidden, grads, xt = forward(by_col, normed, cotangent, weight_tiles, n, list_len, dp_size)
    d, parts = backward(by_row, listed, grads, xt, weight_tiles, n, list_len, rows, dp_size)
    grad_tiles, d_normed, hidden = finish_sum(listed[-1], parts, d, hidden)
    return hidden, d_normed, grad_tiles


def solution(mesh):
    return jax.shard_map(
        local,
        mesh=mesh,
        in_specs=(P(("dp", "tp"), None), P("dp", "tp"), P(None, "tp", None, None), P()),
        out_specs=(P("dp", "tp"), P(("dp", "tp"), None), P(None, "tp", "dp", None)),
        check_vma=False,
    )
```

```python
import functools

import jax
import jax.numpy as jnp
from jax import lax
from jax.experimental import pallas as pl
from jax.experimental.pallas import tpu as pltpu
from jax.sharding import PartitionSpec as P

MESH = pl.DeviceIdType.MESH
VMEM_LIMIT = 67_043_328
CORES = 2
FINE = 4


def ring_width(n):
    width = 2
    while 4 * width * width <= n:
        width *= 2
    return width


def split(value, by):
    if getattr(value, "ndim", 0) and by & (by - 1) == 0:
        return value >> (by.bit_length() - 1), value & (by - 1)
    return value // by, value % by


def ring_pos(index, n):
    y_size = ring_width(n)
    z, y = split(index, y_size)
    inner, _ = split(y + y_size - 1, y_size)
    _, odd = split(z, 2)
    snake = z * (y_size - 1) + (1 - odd) * (y - 1) + odd * (y_size - 1 - y)
    return inner * snake + (1 - inner) * (n - 1 - z)


def ring_index(pos, n):
    y_size = ring_width(n)
    z_size = n // y_size
    back = lax.div(pos, n - z_size)
    z = lax.div(pos, y_size - 1)
    k = lax.rem(pos, y_size - 1)
    odd = lax.rem(z, 2)
    y = (1 - odd) * (k + 1) + odd * (y_size - 1 - k)
    return (1 - back) * (z * y_size + y) + back * (n - 1 - pos) * y_size


def arrival(index, me, n):
    offset = ring_pos(index, n) - ring_pos(me, n)
    offset = jnp.where(offset < 0, offset + n, offset)
    behind = 2 * (n - offset) - 1
    return jnp.where(offset == 0, 0, jnp.where(offset < n // 2, 2 * offset, behind))


def arrival_plan(n, owned):
    base = owned // n
    low, high = base - base // 4, base + base // 4
    chunks, cells, start = [], 4, 0
    for step in range(n // 2 + 1):
        landed = min(2 * step + 1, n)
        stop = max(low * landed, owned - high * (n - landed))
        cells = max(cells, landed - start // high)
        sizes = []
        left = stop - start
        if left > 16:
            sizes.append(8)
            left -= 8
        if left > high:
            sizes.append(left // 8 * 4)
            left -= sizes[-1]
        sizes.append(left)
        for size in sizes:
            chunks.append((step, start, size))
            start += size
    return chunks, cells


class Ring:
    def __init__(self, n):
        self.n = n
        self.half = n // 2
        self.pos = ring_pos(lax.axis_index("tp"), n)

    def at(self, offset):
        return ring_index(lax.rem(self.pos + offset + self.n, self.n), self.n)


def hops(ring, way, piece):
    return ring.half if way == piece else ring.half - 1


def fine_hops(ring, way, quarter):
    return hops(ring, way, quarter // (FINE // 2))


def step_of(way):
    return 1 - 2 * way


def unrolled(count, body):
    by = max(size for size in range(1, 11) if count % size == 0)

    def steps(i, carry):
        for u in range(by):
            body(i * by + u)
        return carry

    lax.fori_loop(0, count // by, steps, 0)


SLOT_F, ROW_F, KEEP_F, LAST_F, SLOT_B, COL_B, KEEP_B, LAST_B, LIST_ROW, LIST_BLOCK = range(10)
GROUP, COL, ROW, KEY_F, KEY_B, KEY_A, SLOT, BLOCK = range(8)


def tile_fields(mine, me, tile_rows, tile_cols, n):
    owned = mine.shape[1]
    cols_dev = tile_cols // n
    row, col = split(mine, tile_cols)
    group, local_col = split(col, cols_dev)
    slots = lax.broadcasted_iota(jnp.int32, mine.shape, 1)
    order = arrival(group, me, n)
    _, cells = arrival_plan(n, owned)
    cell = order
    for _ in range(n // cells + 1):
        cell = jnp.where(cell >= cells, cell - cells, cell)
    return [
        group, local_col, row, col * tile_rows + row, row * tile_cols + col,
        order * owned + slots, slots, cell * cols_dev + local_col,
    ]


def write_tables(dims, me, slot_ref, by_row, tables, rank_ref):
    n, tile_rows, cols_dev, list_len, owned = dims
    mine = slot_ref[:, pl.ds(pl.multiple_of(me * owned, owned), owned)]
    for at, field in enumerate(tile_fields(mine, me, tile_rows, cols_dev * n, n)):
        by_row[at : at + 1, :] = field
    by_col = by_row[...].T

    def across(field):
        return by_row[field : field + 1, :]

    def down(field):
        return by_col[:, field : field + 1]

    def line(count):
        return lax.broadcasted_iota(jnp.int32, (owned, count), 1)

    def put(at, values):
        tables[at : at + 1, : values.shape[1]] = values

    def pick(hit, values):
        return jnp.sum(jnp.where(hit, values, 0), axis=0, keepdims=True)

    same = across(GROUP) == down(GROUP)

    def build(key, sub, n_sub, slot_at, field, field_at, most, keep_at, last_at):
        less = same & (across(key) < down(key))
        pos = jnp.sum(jnp.where(less, 1, 0), axis=1, keepdims=True)
        alike = less & (across(sub) == down(sub))
        keep = jnp.minimum(jnp.sum(jnp.where(alike, 1, 0), axis=1, keepdims=True), 1)
        hit = line(n * list_len) == down(GROUP) * list_len + pos
        put(slot_at, jnp.minimum(pick(hit, down(SLOT)), owned - 1))
        put(field_at, jnp.minimum(pick(hit, down(field)), most))
        put(keep_at, pick(hit, keep))
        inside = line(n * n_sub) == down(GROUP) * n_sub + down(sub)
        last = jnp.max(jnp.where(inside, pos + 1, 0), axis=0, keepdims=True)
        put(last_at, jnp.minimum(last, list_len))

    tables[...] = jnp.zeros(tables.shape, jnp.int32)
    build(KEY_F, COL, cols_dev, SLOT_F, ROW, ROW_F, tile_rows - 1, KEEP_F, LAST_F)
    build(KEY_B, ROW, tile_rows, SLOT_B, COL, COL_B, cols_dev - 1, KEEP_B, LAST_B)
    ahead = across(KEY_A) < down(KEY_A)
    rank = jnp.sum(jnp.where(ahead, 1, 0), axis=1, keepdims=True)
    hit = line(owned) == rank
    _, cells = arrival_plan(n, owned)
    put(LIST_ROW, jnp.minimum(pick(hit, down(ROW)), tile_rows - 1))
    put(LIST_BLOCK, jnp.minimum(pick(hit, down(BLOCK)), cells * cols_dev - 1))
    behind = down(KEY_A) < across(KEY_A)
    rank_ref[...] = jnp.sum(jnp.where(behind, 1, 0), axis=0, keepdims=True)


def step_kernel(dims, plan, big, slot_ref, x_ref, cot_ref, w_ref, *refs):
    n, tile_rows, cols_dev, list_len, rows, tokens, tile, dp_size, owned = dims
    hidden_ref, d_ref, parts_ref, rank_ref, mate, gall = refs[:6]
    (own, xg, ww, buf, acc, send, blocks, xt, stage, dsend, drecv, cot, hid,
     by_row, tables_v, tables,
     x_sem, load_sem, tab_sem, ag_send, ag_recv, rs_send, rs_recv,
     work_sem, g_send, g_recv, p_send, p_recv, t_sem,
     xs_send, xs_recv, x_local, ds_send, ds_recv) = refs[6:]
    ring = Ring(n)
    half = ring.half
    me = lax.axis_index("tp")
    me_dp = lax.axis_index("dp")
    core, x_part = lax.rem(me_dp, CORES), lax.div(me_dp, CORES)
    n_parts = dp_size // CORES
    band = tile // dp_size
    piece_cols = cols_dev // 2
    fine_rows = tile_rows // FINE
    n_stage = stage.shape[0]
    chunks, cells = plan
    partner = {"dp": x_part * CORES + 1 - core}
    seg = buf.shape[0] - 1
    n_seg = list_len // seg
    lower, upper = slice(0, tile), slice(tile, 2 * tile)

    own_rows = pl.ds(pl.multiple_of(me * rows, rows), rows)
    x_loads = [
        pltpu.make_async_copy(
            x_ref.at[:, pl.ds(r * tile, tile)], xg.at[r, own_rows, :], x_sem.at[r]
        )
        for r in range(tile_rows)
    ]
    loads = [
        pltpu.make_async_copy(cot_ref, cot, load_sem.at[0]),
        pltpu.make_async_copy(w_ref.at[0], ww.at[:, :, pl.ds(0, tile)], load_sem.at[1]),
        pltpu.make_async_copy(w_ref.at[1], ww.at[:, :, pl.ds(tile, tile)], load_sem.at[2]),
    ]
    for load in x_loads + loads:
        load.start()

    def x_device(off):
        return {"dp": lax.rem(x_part + off, n_parts) * CORES + core}

    barrier = pltpu.get_barrier_semaphore()
    for offset in (1, -1):
        pl.semaphore_signal(
            barrier, inc=1, device_id={"tp": ring.at(offset)}, device_id_type=MESH
        )
    pl.semaphore_signal(barrier, inc=1, device_id=partner, device_id_type=MESH)
    for off in range(1, n_parts):
        pl.semaphore_signal(barrier, inc=1, device_id=x_device(off), device_id_type=MESH)
    pl.semaphore_wait(barrier, 3 + n_parts - 1)
    for load in x_loads:
        load.wait()

    def token_copy(way, piece, hop):
        shard = ring.at(-step_of(way) * hop)
        view = xg.at[
            pl.ds(piece * fine_rows, fine_rows),
            pl.ds(pl.multiple_of(shard * rows, rows), rows),
            :,
        ]
        return pltpu.make_async_remote_copy(
            src_ref=view, dst_ref=view,
            send_sem=ag_send.at[way, piece, hop], recv_sem=ag_recv.at[way, piece, hop],
            device_id={"tp": ring.at(step_of(way))}, device_id_type=MESH,
        )

    lanes = [(0, 0), (1, 1), (0, 1), (1, 0)]
    fine_lanes = []
    for q in range(FINE):
        fine_lanes += [(0, q), (1, FINE - 1 - q)]
    for way, piece in fine_lanes:
        token_copy(way, piece, 0).start()
    write_tables(
        (n, tile_rows, cols_dev, list_len, owned), me, slot_ref, by_row, tables_v, rank_ref
    )
    for hop in range(half):
        for way, piece in fine_lanes:
            if hop < fine_hops(ring, way, piece):
                token_copy(way, piece, hop).wait_recv()
                if hop + 1 < fine_hops(ring, way, piece):
                    token_copy(way, piece, hop + 1).start()
        if hop == 0:
            table_copy = pltpu.make_async_copy(tables_v, tables, tab_sem.at[0])
            table_copy.start()
    table_copy.wait()
    loads[1].wait()
    loads[2].wait()

    def part_at(which, c, m):
        return (which * cols_dev + c) * 2 + m

    def compute(which, dest):
        buf[0] = jnp.zeros(buf.shape[1:], buf.dtype)
        for s in range(n_seg):
            if s > 0:
                buf[0] = buf[seg]

            def tile_step(j):
                at = dest * list_len + s * seg + j
                term = jnp.dot(
                    xg[tables[ROW_F, at]], ww[tables[SLOT_F, at]],
                    preferred_element_type=jnp.float32,
                )
                buf[j + 1] = term + jnp.where(tables[KEEP_F, at] > 0, buf[j], 0.0)

            unrolled(seg, tile_step)

            def column(c, carry):
                last = tables[LAST_F, dest * cols_dev + c]
                value = buf[jnp.clip(last - s * seg, 0, seg)]
                for m, side in enumerate((lower, upper)):
                    new = value[:, side]
                    if s > 0:
                        new = jnp.where(last > s * seg, new, acc[part_at(which, c, m)])
                    acc[part_at(which, c, m)] = new
                return carry

            lax.fori_loop(0, cols_dev, column, 0)

    def landing(way, piece, hop):
        return ((way * 2 + piece) * half + hop) * piece_cols

    def sum_copy(way, piece, hop):
        return pltpu.make_async_remote_copy(
            src_ref=send.at[way, piece, hop % 2],
            dst_ref=blocks.at[pl.ds(landing(way, piece, hop), piece_cols)],
            send_sem=rs_send.at[way, piece, hop], recv_sem=rs_recv.at[way, piece, hop],
            device_id={"tp": ring.at(step_of(way))}, device_id_type=MESH,
        )

    def first_hop(way, piece):
        return half - hops(ring, way, piece)

    def push(which, way, piece, hop):
        fresh = hop == first_hop(way, piece)
        if hop - 2 >= first_hop(way, piece):
            sum_copy(way, piece, hop - 2).wait_send()
        if not fresh:
            sum_copy(way, piece, hop - 1).wait_recv()

        def column(c, carry):
            for m, side in enumerate((lower, upper)):
                value = acc[part_at(which, piece * piece_cols + c, m)]
                if not fresh:
                    arrived = blocks[landing(way, piece, hop - 1) + c, :, side]
                    value = value + arrived.astype(jnp.float32)
                send[way, piece, hop % 2, c, :, side] = value.astype(jnp.bfloat16)
            return carry

        lax.fori_loop(0, piece_cols, column, 0)
        sum_copy(way, piece, hop).start()

    compute(0, ring.at(half))
    push(0, 0, 0, 0)
    push(0, 1, 1, 0)
    for hop in range(1, half):
        compute(0, ring.at(half - hop))
        compute(1, ring.at(hop - half))
        push(0, 0, 1, hop)
        push(1, 1, 0, hop)
        push(0, 0, 0, hop)
        push(1, 1, 1, hop)
    compute(0, me)

    order = lax.broadcasted_iota(jnp.int32, (tile, tile), 0)
    source = lax.broadcasted_iota(jnp.int32, (tile, tile), 1)
    for_core = (order // (n_parts * band) + core) % CORES
    for_part = order // band % n_parts
    perm = (source == (for_part * CORES + for_core) * band + order % band)
    perm = jnp.where(perm, 1.0, 0.0).astype(jnp.bfloat16)
    half_tile = tile // CORES

    def transpose_block(r):
        turned = lax.dot_general(
            perm, xg[r], (((1,), (1,)), ((), ())), preferred_element_type=jnp.float32
        ).astype(jnp.bfloat16)
        xt[0, r] = turned[:half_tile]
        xt[2, r] = turned[half_tile:]

    unrolled(tile_rows, transpose_block)
    turned_copy = pltpu.make_async_remote_copy(
        src_ref=xt.at[2], dst_ref=xt.at[1],
        send_sem=t_sem.at[0], recv_sem=t_sem.at[1],
        device_id=partner, device_id_type=MESH,
    )
    turned_copy.start()
    loads[0].wait()

    def piece_slice(shard, piece):
        start = pl.multiple_of(shard * cols_dev + piece * piece_cols, piece_cols)
        return pl.ds(start, piece_cols)

    def own_piece(piece):
        return own.at[pl.ds(piece * piece_cols, piece_cols)]

    def grad_copy(way, piece, hop):
        where = piece_slice(ring.at(-step_of(way) * hop), piece)
        return pltpu.make_async_remote_copy(
            src_ref=gall.at[where] if hop else own_piece(piece), dst_ref=gall.at[where],
            send_sem=g_send.at[way, piece, hop], recv_sem=g_recv.at[way, piece, hop],
            device_id={"tp": ring.at(step_of(way))}, device_id_type=MESH,
        )

    def pair_copy(offset, piece):
        where = piece_slice(ring.at(offset), piece)
        g = offset % n
        return pltpu.make_async_remote_copy(
            src_ref=gall.at[where] if offset else own_piece(piece), dst_ref=mate.at[where],
            send_sem=p_send.at[g, piece], recv_sem=p_recv.at[g, piece],
            device_id=partner, device_id_type=MESH,
        )

    def gate_piece(piece):
        for way in range(2):
            sum_copy(way, piece, half - 1).wait_recv()
        for k in range(piece_cols):
            c = piece * piece_cols + k
            gate, up = (
                acc[part_at(0, c, m)]
                + blocks[landing(0, piece, half - 1) + k, :, side].astype(jnp.float32)
                + blocks[landing(1, piece, half - 1) + k, :, side].astype(jnp.float32)
                for m, side in enumerate((lower, upper))
            )
            s = jax.nn.sigmoid(gate)
            act = gate * s
            columns = slice(c * tile, (c + 1) * tile)
            cotangent = cot[:, columns].astype(jnp.float32)
            hid[:, columns] = (act * up).astype(jnp.bfloat16)
            own[c, :, lower] = (
                cotangent * up * (s * (1.0 + gate * (1.0 - s)))
            ).astype(jnp.bfloat16)
            own[c, :, upper] = (cotangent * act).astype(jnp.bfloat16)

    gate_piece(0)
    grad_copy(0, 0, 0).start()
    gate_piece(1)
    for way, piece in lanes[1:]:
        grad_copy(way, piece, 0).start()
    for piece in range(2):
        pair_copy(0, piece).start()
    hidden_copy = pltpu.make_async_copy(hid, hidden_ref, load_sem.at[3])
    hidden_copy.start()

    def clear(r):
        acc[r] = jnp.zeros(acc.shape[1:], acc.dtype)

    unrolled(tile_rows, clear)
    turned_copy.wait()

    def x_copy(i, off):
        _, start, size = chunks[i]
        dest = lax.rem(x_part + off, n_parts)
        return pltpu.make_async_remote_copy(
            src_ref=stage.at[i % n_stage, dest, pl.ds(0, size)],
            dst_ref=parts_ref.at[x_part, pl.ds(start, size)],
            send_sem=xs_send.at[i, off - 1], recv_sem=xs_recv.at[i, off - 1],
            device_id=x_device(off), device_id_type=MESH,
        )

    def keep_copy(i):
        _, start, size = chunks[i]
        return pltpu.make_async_copy(
            stage.at[i % n_stage, x_part, pl.ds(0, size)],
            parts_ref.at[x_part, pl.ds(start, size)],
            x_local.at[i],
        )

    def finish(i):
        for off in range(1, n_parts):
            x_copy(i, off).wait_send()
        keep_copy(i).wait()

    offsets = [0]
    for hop in range(1, half):
        offsets += [-hop, hop]
    offsets.append(half)
    side_blocks = cells * cols_dev

    def cell_of(offset):
        return offsets.index(offset) % cells * cols_dev

    def landed(step):
        return [offset for offset in offsets if abs(offset) == step]

    def fill(step, side):
        copies = []
        for number, offset in enumerate(landed(step)):
            for piece in range(2):
                if side:
                    pair_copy(offset, piece).wait_recv()
                    ref = mate.at[piece_slice(ring.at(offset), piece)]
                elif offset:
                    ref = gall.at[piece_slice(ring.at(offset), piece)]
                else:
                    ref = own_piece(piece)
                first = side * side_blocks + cell_of(offset) + piece * piece_cols
                copies.append(
                    pltpu.make_async_copy(
                        ref, blocks.at[pl.ds(first, piece_cols)],
                        work_sem.at[number, side, piece],
                    )
                )
                copies[-1].start()
        return copies

    def settle(copies):
        for copy in copies:
            copy.wait()

    def weight_grads(step, which=None):
        at_this = [i for i, chunk in enumerate(chunks) if chunk[0] == step]
        for i in at_this if which is None else at_this[which : which + 1]:
            _, start, size = chunks[i]
            if i >= n_stage:
                finish(i - n_stage)
            slot = i % n_stage

            def outer(j):
                r, block = tables[LIST_ROW, start + j], tables[LIST_BLOCK, start + j]
                value = jnp.dot(
                    xt[0, r], blocks[block], preferred_element_type=jnp.float32
                ) + jnp.dot(
                    xt[1, r], blocks[side_blocks + block], preferred_element_type=jnp.float32
                )
                for k in range(n_parts):
                    stage[slot, k, j] = value[k * band : (k + 1) * band].astype(jnp.bfloat16)

            unrolled(size, outer)
            for off in range(1, n_parts):
                x_copy(i, off).start()
            keep_copy(i).start()

    def token_grads(offset, source=None):
        shard = ring.at(offset)
        source = blocks if source is None else source
        cell = cell_of(offset) if source is blocks else shard * cols_dev
        buf[0] = jnp.zeros(buf.shape[1:], buf.dtype)
        for s, side in zip(range(n_seg), (lower, upper)):
            if s > 0:
                buf[0, :, side] = buf[seg, :, lower]

            def back(j):
                at = shard * list_len + s * seg + j
                term = lax.dot_general(
                    source[cell + tables[COL_B, at]], ww[tables[SLOT_B, at]],
                    (((1,), (1,)), ((), ())), preferred_element_type=jnp.float32,
                )
                kept = jnp.where(tables[KEEP_B, at] > 0, buf[j, :, side], 0.0)
                buf[j + 1, :, side] = term + kept

            unrolled(seg, back)

        def add_row(r):
            last = tables[LAST_B, shard * tile_rows + r]
            value = buf[jnp.minimum(last, seg), :, lower]
            if n_seg > 1:
                later = buf[jnp.maximum(last - seg, 0), :, upper]
                value = jnp.where(last > seg, later, value)
            acc[r] += value

        unrolled(tile_rows, add_row)

    def arrive(way, piece, hop):
        if hop >= hops(ring, way, piece):
            return
        grad_copy(way, piece, hop).wait_recv()
        if hop + 1 < hops(ring, way, piece):
            grad_copy(way, piece, hop + 1).start()
        pair_copy(-step_of(way) * (hop + 1), piece).start()

    settle(fill(0, 0))
    settle(fill(0, 1))
    weight_grads(0)
    token_grads(0)
    for hop in range(half - 1):
        arrive(0, 0, hop)
        arrive(1, 1, hop)
        if hop > 0:
            token_grads(-hop)
            token_grads(hop)
        arrive(0, 1, hop)
        arrive(1, 0, hop)
        settle(fill(hop + 1, 0) + fill(hop + 1, 1))
        if hop < half - 2:
            weight_grads(hop + 1)
    last = half - 1
    n_last = len([chunk for chunk in chunks if chunk[0] == last])
    n_half = len([chunk for chunk in chunks if chunk[0] == half])
    weight_grads(last, 0)
    token_grads(-last)
    for which in range(1, n_last):
        weight_grads(last, which)
    token_grads(last)
    arrive(0, 0, last)
    arrive(1, 1, last)
    if big:
        settle(fill(half, 0))
        fills = []
        token_grads(half)
    else:
        fills = fill(half, 0)
        token_grads(half, gall)

    def d_copy(way, piece, hop):
        return pltpu.make_async_remote_copy(
            src_ref=dsend.at[way, piece, hop], dst_ref=drecv.at[way, piece, hop],
            send_sem=ds_send.at[way, piece, hop], recv_sem=ds_recv.at[way, piece, hop],
            device_id={"tp": ring.at(step_of(way))}, device_id_type=MESH,
        )

    def own_term(dest, piece):
        return acc[
            pl.ds(piece * fine_rows, fine_rows),
            pl.ds(pl.multiple_of(dest * rows, rows), rows),
            :,
        ]

    def d_first(way, piece):
        return half - fine_hops(ring, way, piece)

    def d_push(way, piece, hop):
        value = own_term(ring.at(step_of(way) * (half - hop)), piece)
        if hop > d_first(way, piece):
            d_copy(way, piece, hop - 1).wait_recv()
            value = value + drecv[way, piece, hop - 1].astype(jnp.float32)
        dsend[way, piece, hop] = value.astype(jnp.bfloat16)
        d_copy(way, piece, hop).start()

    for hop in range(half):
        fresh = [lane for lane in fine_lanes if hop == d_first(*lane)]
        going = [lane for lane in fine_lanes if hop > d_first(*lane)]
        for way, piece in fresh + going:
            d_push(way, piece, hop)
        if hop == 0:
            settle(fills + fill(half, 1))
        if hop < n_half:
            weight_grads(half, hop)
    for piece in range(FINE):
        for way in range(2):
            d_copy(way, piece, half - 1).wait_recv()
        d_ref[pl.ds(piece * fine_rows, fine_rows)] = (
            own_term(me, piece)
            + drecv[0, piece, half - 1].astype(jnp.float32)
            + drecv[1, piece, half - 1].astype(jnp.float32)
        ).astype(jnp.bfloat16)

    for i in range(max(0, len(chunks) - n_stage), len(chunks)):
        finish(i)
    for i in range(len(chunks)):
        for off in range(1, n_parts):
            x_copy(i, off).wait_recv()
    for way, piece in lanes:
        for hop in range(hops(ring, way, piece)):
            grad_copy(way, piece, hop).wait_send()
        for hop in range(max(first_hop(way, piece), half - 2), half):
            sum_copy(way, piece, hop).wait_send()
    for way, piece in fine_lanes:
        for hop in range(fine_hops(ring, way, piece)):
            token_copy(way, piece, hop).wait_send()
        for hop in range(d_first(way, piece), half):
            d_copy(way, piece, hop).wait_send()
    for offset in offsets:
        for piece in range(2):
            pair_copy(offset, piece).wait_send()
    hidden_copy.wait()


def step(slot_tile, normed, cotangent, weights, n, list_len, dp_size):
    rows, width = normed.shape
    owned, tile = weights.shape[1:3]
    tile_rows = width // tile
    tokens, cols = cotangent.shape
    cols_dev = cols // tile
    pair = 2 * tile
    half = n // 2
    band = tile // dp_size
    n_parts = dp_size // CORES
    n_stage = 4
    chunks, cells = plan = arrival_plan(n, owned)
    largest = max(size for _, _, size in chunks)
    dims = (n, tile_rows, cols_dev, list_len, rows, tokens, tile, dp_size, owned)
    hbm = pl.BlockSpec(memory_space=pl.ANY)
    vmem = pl.BlockSpec(memory_space=pltpu.VMEM)
    sem = pltpu.SemaphoreType.DMA
    gall_shape = (n * cols_dev, tokens, pair)
    big = n * cols_dev * tokens * pair * 2 > 12 * 2**20
    seg = list_len // 2 if list_len % 8 == 0 else list_len
    most = -(-max(n * list_len, n * tile_rows, owned) // tile) * tile
    d_slots = (2, FINE, half, tile_rows // FINE, rows, tile)
    out_specs = [hbm, vmem, hbm, vmem, hbm]
    out_shape = [
        jax.ShapeDtypeStruct((tokens, cols), jnp.bfloat16),
        jax.ShapeDtypeStruct((tile_rows, rows, tile), jnp.bfloat16),
        jax.ShapeDtypeStruct((n_parts, owned, band, pair), jnp.bfloat16),
        jax.ShapeDtypeStruct((1, owned), jnp.int32),
        jax.ShapeDtypeStruct(gall_shape, jnp.bfloat16),
    ]
    scratch = []
    if big:
        out_specs.append(hbm)
        out_shape.append(jax.ShapeDtypeStruct(gall_shape, jnp.bfloat16))
    else:
        scratch.append(pltpu.VMEM(gall_shape, jnp.bfloat16))
    n_blocks = max(4 * half * (cols_dev // 2), 2 * cells * cols_dev)
    scratch += [
        pltpu.VMEM((cols_dev, tokens, pair), jnp.bfloat16),
        pltpu.VMEM((tile_rows, tokens, tile), jnp.bfloat16),
        pltpu.VMEM((owned, tile, pair), jnp.bfloat16),
        pltpu.VMEM((seg + 1, tokens, pair), jnp.float32),
        pltpu.VMEM((max(4 * cols_dev, tile_rows), tokens, tile), jnp.float32),
        pltpu.VMEM((2, 2, 2, cols_dev // 2, tokens, pair), jnp.bfloat16),
        pltpu.VMEM((n_blocks, tokens, pair), jnp.bfloat16),
        pltpu.VMEM((3, tile_rows, tile // CORES, tokens), jnp.bfloat16),
        pltpu.VMEM((n_stage, n_parts, largest, band, pair), jnp.bfloat16),
        pltpu.VMEM(d_slots, jnp.bfloat16),
        pltpu.VMEM(d_slots, jnp.bfloat16),
        pltpu.VMEM((tokens, cols), jnp.bfloat16),
        pltpu.VMEM((tokens, cols), jnp.bfloat16),
        pltpu.VMEM((8, owned), jnp.int32),
        pltpu.VMEM((16, most), jnp.int32),
        pltpu.SMEM((16, most), jnp.int32),
        sem((tile_rows,)), sem((4,)), sem((1,)),
        sem((2, FINE, half)), sem((2, FINE, half)), sem((2, 2, half)), sem((2, 2, half)),
        sem((2, 2, 2)), sem((2, 2, half)), sem((2, 2, half)),
        sem((n, 2)), sem((n, 2)), sem((2,)),
        sem((len(chunks), n_parts - 1)), sem((len(chunks), n_parts - 1)), sem((len(chunks),)),
        sem((2, FINE, half)), sem((2, FINE, half)),
    ]
    results = pl.pallas_call(
        functools.partial(step_kernel, dims, plan, big),
        name="step",
        in_specs=[vmem, hbm, hbm, hbm],
        out_specs=out_specs,
        out_shape=out_shape,
        scratch_shapes=scratch,
        compiler_params=pltpu.CompilerParams(
            collective_id=0, has_side_effects=True, vmem_limit_bytes=VMEM_LIMIT
        ),
    )(slot_tile.reshape(1, -1), normed, cotangent, weights)
    return results[:4]


def finish_kernel(place_ref, parts_ref, d_ref, hidden_ref, out_ref, d_out, hidden_out):
    n_parts = parts_ref.shape[0]
    _, chunk, _, tile = out_ref.shape
    base = pl.program_id(0) * chunk

    @pl.when(pl.program_id(0) == 0)
    def _():
        for r in range(d_ref.shape[0]):
            d_out[:, r * tile : (r + 1) * tile] = d_ref[r]

    hidden_out[...] = hidden_ref[...]

    def one(p):
        at = place_ref[base + p]
        total = parts_ref[0, at].astype(jnp.float32)
        for k in range(1, n_parts):
            total = total + parts_ref[k, at].astype(jnp.float32)
        out_ref[0, p] = total[:, :tile]
        out_ref[1, p] = total[:, tile:]

    unrolled(chunk, one)


def finish_sum(place, parts, d, hidden):
    owned = place.shape[0]
    n_parts, listed, band, pair = parts.shape
    tile = pair // 2
    tile_rows, rows, _ = d.shape
    tokens, cols = hidden.shape
    steps = 2
    return pl.pallas_call(
        finish_kernel,
        name="finish",
        grid=(steps,),
        in_specs=[
            pl.BlockSpec(memory_space=pltpu.SMEM),
            pl.BlockSpec((n_parts, listed, band, pair), lambda i: (0, 0, 0, 0)),
            pl.BlockSpec((tile_rows, rows, tile), lambda i: (0, 0, 0)),
            pl.BlockSpec((tokens // steps, cols), lambda i: (i, 0)),
        ],
        out_specs=[
            pl.BlockSpec((2, owned // steps, band, tile), lambda i: (0, i, 0, 0)),
            pl.BlockSpec((rows, tile_rows * tile), lambda i: (0, 0)),
            pl.BlockSpec((tokens // steps, cols), lambda i: (i, 0)),
        ],
        out_shape=[
            jax.ShapeDtypeStruct((2, owned, band, tile), jnp.float32),
            jax.ShapeDtypeStruct((rows, tile_rows * tile), d.dtype),
            jax.ShapeDtypeStruct(hidden.shape, hidden.dtype),
        ],
        compiler_params=pltpu.CompilerParams(vmem_limit_bytes=VMEM_LIMIT),
    )(place, parts, d, hidden)


def local(normed, cotangent, weight_tiles, slot_tile):
    n = lax.axis_size("tp")
    dp_size = lax.axis_size("dp")
    owned = weight_tiles.shape[1]
    base_count = owned // n
    list_len = base_count + base_count // 4
    hidden, d, parts, rank = step(
        slot_tile, normed, cotangent, weight_tiles, n, list_len, dp_size
    )
    grad_tiles, d_normed, hidden = finish_sum(rank.reshape(owned), parts, d, hidden)
    return hidden, d_normed, grad_tiles


def solution(mesh):
    return jax.shard_map(
        local,
        mesh=mesh,
        in_specs=(P(("dp", "tp"), None), P("dp", "tp"), P(None, "tp", None, None), P()),
        out_specs=(P("dp", "tp"), P(("dp", "tp"), None), P(None, "tp", "dp", None)),
        check_vma=False,
    )
```

```python
import functools

import jax
import jax.numpy as jnp
from jax import lax
from jax.experimental import pallas as pl
from jax.experimental.pallas import tpu as pltpu
from jax.sharding import PartitionSpec as P

MESH = pl.DeviceIdType.MESH
VMEM_LIMIT = 67_043_328
CORES = 2
FINE = 4


def ring_width(n):
    width = 2
    while 4 * width * width <= n:
        width *= 2
    return width


def split(value, by):
    if getattr(value, "ndim", 0) and by & (by - 1) == 0:
        return value >> (by.bit_length() - 1), value & (by - 1)
    return value // by, value % by


def ring_pos(index, n):
    y_size = ring_width(n)
    z, y = split(index, y_size)
    inner, _ = split(y + y_size - 1, y_size)
    _, odd = split(z, 2)
    snake = z * (y_size - 1) + (1 - odd) * (y - 1) + odd * (y_size - 1 - y)
    return inner * snake + (1 - inner) * (n - 1 - z)


def ring_index(pos, n):
    y_size = ring_width(n)
    z_size = n // y_size
    back = lax.div(pos, n - z_size)
    z = lax.div(pos, y_size - 1)
    k = lax.rem(pos, y_size - 1)
    odd = lax.rem(z, 2)
    y = (1 - odd) * (k + 1) + odd * (y_size - 1 - k)
    return (1 - back) * (z * y_size + y) + back * (n - 1 - pos) * y_size


def arrival(index, me, n):
    offset = ring_pos(index, n) - ring_pos(me, n)
    offset = jnp.where(offset < 0, offset + n, offset)
    behind = 2 * (n - offset) - 1
    return jnp.where(offset == 0, 0, jnp.where(offset < n // 2, 2 * offset, behind))


def arrival_plan(n, owned):
    base = owned // n
    low, high = base - base // 4, base + base // 4
    chunks, cells, start = [], 4, 0
    for step in range(n // 2 + 1):
        landed = min(2 * step + 1, n)
        stop = max(low * landed, owned - high * (n - landed))
        cells = max(cells, landed - start // high)
        sizes = []
        left = stop - start
        if left > 16:
            sizes.append(8)
            left -= 8
        if left > high:
            sizes.append(left // 8 * 4)
            left -= sizes[-1]
        sizes.append(left)
        for size in sizes:
            chunks.append((step, start, size))
            start += size
    return chunks, cells


class Ring:
    def __init__(self, n):
        self.n = n
        self.half = n // 2
        self.pos = ring_pos(lax.axis_index("tp"), n)

    def at(self, offset):
        return ring_index(lax.rem(self.pos + offset + self.n, self.n), self.n)


def hops(ring, way, piece):
    return ring.half if way == piece else ring.half - 1


def fine_hops(ring, way, quarter):
    return hops(ring, way, quarter // (FINE // 2))


def step_of(way):
    return 1 - 2 * way


def unrolled(count, body):
    by = max(size for size in range(1, 11) if count % size == 0)

    def steps(i, carry):
        for u in range(by):
            body(i * by + u)
        return carry

    lax.fori_loop(0, count // by, steps, 0)


SLOT_F, ROW_F, KEEP_F, LAST_F, SLOT_B, COL_B, KEEP_B, LAST_B, LIST_ROW, LIST_BLOCK = range(10)
GROUP, COL, ROW, KEY_F, KEY_B, KEY_A, SLOT, BLOCK = range(8)


def tile_fields(mine, me, tile_rows, tile_cols, n):
    owned = mine.shape[1]
    cols_dev = tile_cols // n
    row, col = split(mine, tile_cols)
    group, local_col = split(col, cols_dev)
    slots = lax.broadcasted_iota(jnp.int32, mine.shape, 1)
    order = arrival(group, me, n)
    _, cells = arrival_plan(n, owned)
    cell = order
    for _ in range(n // cells + 1):
        cell = jnp.where(cell >= cells, cell - cells, cell)
    return [
        group, local_col, row, col * tile_rows + row, row * tile_cols + col,
        order * owned + slots, slots, cell * cols_dev + local_col,
    ]


def write_tables(dims, me, slot_ref, by_row, tables, rank_ref):
    n, tile_rows, cols_dev, list_len, owned = dims
    mine = slot_ref[:, pl.ds(pl.multiple_of(me * owned, owned), owned)]
    for at, field in enumerate(tile_fields(mine, me, tile_rows, cols_dev * n, n)):
        by_row[at : at + 1, :] = field
    by_col = by_row[...].T

    def across(field):
        return by_row[field : field + 1, :]

    def down(field):
        return by_col[:, field : field + 1]

    def line(count):
        return lax.broadcasted_iota(jnp.int32, (owned, count), 1)

    def put(at, values):
        tables[at : at + 1, : values.shape[1]] = values

    def pick(hit, values):
        return jnp.sum(jnp.where(hit, values, 0), axis=0, keepdims=True)

    same = across(GROUP) == down(GROUP)

    def build(key, sub, n_sub, slot_at, field, field_at, most, keep_at, last_at):
        less = same & (across(key) < down(key))
        pos = jnp.sum(jnp.where(less, 1, 0), axis=1, keepdims=True)
        alike = less & (across(sub) == down(sub))
        keep = jnp.minimum(jnp.sum(jnp.where(alike, 1, 0), axis=1, keepdims=True), 1)
        hit = line(n * list_len) == down(GROUP) * list_len + pos
        put(slot_at, jnp.minimum(pick(hit, down(SLOT)), owned - 1))
        put(field_at, jnp.minimum(pick(hit, down(field)), most))
        put(keep_at, pick(hit, keep))
        inside = line(n * n_sub) == down(GROUP) * n_sub + down(sub)
        last = jnp.max(jnp.where(inside, pos + 1, 0), axis=0, keepdims=True)
        put(last_at, jnp.minimum(last, list_len))

    tables[...] = jnp.zeros(tables.shape, jnp.int32)
    build(KEY_F, COL, cols_dev, SLOT_F, ROW, ROW_F, tile_rows - 1, KEEP_F, LAST_F)
    build(KEY_B, ROW, tile_rows, SLOT_B, COL, COL_B, cols_dev - 1, KEEP_B, LAST_B)
    ahead = across(KEY_A) < down(KEY_A)
    rank = jnp.sum(jnp.where(ahead, 1, 0), axis=1, keepdims=True)
    hit = line(owned) == rank
    _, cells = arrival_plan(n, owned)
    put(LIST_ROW, jnp.minimum(pick(hit, down(ROW)), tile_rows - 1))
    put(LIST_BLOCK, jnp.minimum(pick(hit, down(BLOCK)), cells * cols_dev - 1))
    behind = down(KEY_A) < across(KEY_A)
    rank_ref[...] = jnp.sum(jnp.where(behind, 1, 0), axis=0, keepdims=True)


def step_kernel(dims, plan, big, slot_ref, x_ref, cot_ref, w_ref, *refs):
    n, tile_rows, cols_dev, list_len, rows, tokens, tile, dp_size, owned = dims
    hidden_ref, d_ref, parts_ref, rank_ref, mate, gall = refs[:6]
    (own, xg, ww, buf, acc, send, blocks, xt, stage, dsend, drecv, cot, hid,
     by_row, tables_v, tables,
     x_sem, load_sem, tab_sem, ag_send, ag_recv, rs_send, rs_recv,
     work_sem, g_send, g_recv, p_send, p_recv, t_sem,
     xs_send, xs_recv, x_local, ds_send, ds_recv) = refs[6:]
    ring = Ring(n)
    half = ring.half
    me = lax.axis_index("tp")
    me_dp = lax.axis_index("dp")
    core, x_part = lax.rem(me_dp, CORES), lax.div(me_dp, CORES)
    n_parts = dp_size // CORES
    band = tile // dp_size
    piece_cols = cols_dev // 2
    fine_rows = tile_rows // FINE
    n_stage = stage.shape[0]
    chunks, cells = plan
    partner = {"dp": x_part * CORES + 1 - core}
    seg = buf.shape[0] - 1
    n_seg = list_len // seg
    lower, upper = slice(0, tile), slice(tile, 2 * tile)

    own_rows = pl.ds(pl.multiple_of(me * rows, rows), rows)
    x_loads = [
        pltpu.make_async_copy(
            x_ref.at[:, pl.ds(r * tile, tile)], xg.at[r, own_rows, :], x_sem.at[r]
        )
        for r in range(tile_rows)
    ]
    loads = [
        pltpu.make_async_copy(cot_ref, cot, load_sem.at[0]),
        pltpu.make_async_copy(w_ref.at[0], ww.at[:, :, pl.ds(0, tile)], load_sem.at[1]),
        pltpu.make_async_copy(w_ref.at[1], ww.at[:, :, pl.ds(tile, tile)], load_sem.at[2]),
    ]
    for load in x_loads + loads:
        load.start()

    def x_device(off):
        return {"dp": lax.rem(x_part + off, n_parts) * CORES + core}

    barrier = pltpu.get_barrier_semaphore()
    for offset in (1, -1):
        pl.semaphore_signal(
            barrier, inc=1, device_id={"tp": ring.at(offset)}, device_id_type=MESH
        )
    pl.semaphore_signal(barrier, inc=1, device_id=partner, device_id_type=MESH)
    for off in range(1, n_parts):
        pl.semaphore_signal(barrier, inc=1, device_id=x_device(off), device_id_type=MESH)
    pl.semaphore_wait(barrier, 3 + n_parts - 1)
    def token_copy(way, piece, hop):
        shard = ring.at(-step_of(way) * hop)
        view = xg.at[
            pl.ds(piece * fine_rows, fine_rows),
            pl.ds(pl.multiple_of(shard * rows, rows), rows),
            :,
        ]
        return pltpu.make_async_remote_copy(
            src_ref=view, dst_ref=view,
            send_sem=ag_send.at[way, piece, hop], recv_sem=ag_recv.at[way, piece, hop],
            device_id={"tp": ring.at(step_of(way))}, device_id_type=MESH,
        )

    lanes = [(0, 0), (1, 1), (0, 1), (1, 0)]
    fine_lanes = []
    for q in range(FINE):
        fine_lanes += [(0, q), (1, FINE - 1 - q)]
    loaded = set()
    for way, piece in fine_lanes:
        if piece not in loaded:
            for load in x_loads[piece * fine_rows : (piece + 1) * fine_rows]:
                load.wait()
            loaded.add(piece)
        token_copy(way, piece, 0).start()
    write_tables(
        (n, tile_rows, cols_dev, list_len, owned), me, slot_ref, by_row, tables_v, rank_ref
    )
    for hop in range(half):
        for way, piece in fine_lanes:
            if hop < fine_hops(ring, way, piece):
                token_copy(way, piece, hop).wait_recv()
                if hop + 1 < fine_hops(ring, way, piece):
                    token_copy(way, piece, hop + 1).start()
        if hop == 0:
            table_copy = pltpu.make_async_copy(tables_v, tables, tab_sem.at[0])
            table_copy.start()
    table_copy.wait()
    loads[1].wait()
    loads[2].wait()

    def part_at(which, c, m):
        return (which * cols_dev + c) * 2 + m

    def compute(which, dest):
        buf[0] = jnp.zeros(buf.shape[1:], buf.dtype)
        for s in range(n_seg):
            if s > 0:
                buf[0] = buf[seg]

            def tile_step(j):
                at = dest * list_len + s * seg + j
                term = jnp.dot(
                    xg[tables[ROW_F, at]], ww[tables[SLOT_F, at]],
                    preferred_element_type=jnp.float32,
                )
                buf[j + 1] = term + jnp.where(tables[KEEP_F, at] > 0, buf[j], 0.0)

            unrolled(seg, tile_step)

            def column(c, carry):
                last = tables[LAST_F, dest * cols_dev + c]
                value = buf[jnp.clip(last - s * seg, 0, seg)]
                for m, side in enumerate((lower, upper)):
                    new = value[:, side]
                    if s > 0:
                        new = jnp.where(last > s * seg, new, acc[part_at(which, c, m)])
                    acc[part_at(which, c, m)] = new
                return carry

            lax.fori_loop(0, cols_dev, column, 0)

    def landing(way, piece, hop):
        return ((way * 2 + piece) * half + hop) * piece_cols

    def sum_copy(way, piece, hop):
        return pltpu.make_async_remote_copy(
            src_ref=send.at[way, piece, hop % 2],
            dst_ref=blocks.at[pl.ds(landing(way, piece, hop), piece_cols)],
            send_sem=rs_send.at[way, piece, hop], recv_sem=rs_recv.at[way, piece, hop],
            device_id={"tp": ring.at(step_of(way))}, device_id_type=MESH,
        )

    def first_hop(way, piece):
        return half - hops(ring, way, piece)

    def push(which, way, piece, hop):
        fresh = hop == first_hop(way, piece)
        if hop - 2 >= first_hop(way, piece):
            sum_copy(way, piece, hop - 2).wait_send()
        if not fresh:
            sum_copy(way, piece, hop - 1).wait_recv()

        def column(c, carry):
            for m, side in enumerate((lower, upper)):
                value = acc[part_at(which, piece * piece_cols + c, m)]
                if not fresh:
                    arrived = blocks[landing(way, piece, hop - 1) + c, :, side]
                    value = value + arrived.astype(jnp.float32)
                send[way, piece, hop % 2, c, :, side] = value.astype(jnp.bfloat16)
            return carry

        lax.fori_loop(0, piece_cols, column, 0)
        sum_copy(way, piece, hop).start()

    compute(0, ring.at(half))
    push(0, 0, 0, 0)
    push(0, 1, 1, 0)
    for hop in range(1, half):
        compute(0, ring.at(half - hop))
        compute(1, ring.at(hop - half))
        push(0, 0, 1, hop)
        push(1, 1, 0, hop)
        push(0, 0, 0, hop)
        push(1, 1, 1, hop)
    compute(0, me)

    order = lax.broadcasted_iota(jnp.int32, (tile, tile), 0)
    source = lax.broadcasted_iota(jnp.int32, (tile, tile), 1)
    for_core = (order // (n_parts * band) + core) % CORES
    for_part = order // band % n_parts
    perm = (source == (for_part * CORES + for_core) * band + order % band)
    perm = jnp.where(perm, 1.0, 0.0).astype(jnp.bfloat16)
    half_tile = tile // CORES

    def transpose_block(r):
        turned = lax.dot_general(
            perm, xg[r], (((1,), (1,)), ((), ())), preferred_element_type=jnp.float32
        ).astype(jnp.bfloat16)
        xt[0, r] = turned[:half_tile]
        xt[2, r] = turned[half_tile:]

    unrolled(tile_rows, transpose_block)
    turned_copy = pltpu.make_async_remote_copy(
        src_ref=xt.at[2], dst_ref=xt.at[1],
        send_sem=t_sem.at[0], recv_sem=t_sem.at[1],
        device_id=partner, device_id_type=MESH,
    )
    turned_copy.start()
    loads[0].wait()

    def piece_slice(shard, piece):
        start = pl.multiple_of(shard * cols_dev + piece * piece_cols, piece_cols)
        return pl.ds(start, piece_cols)

    def own_piece(piece):
        return own.at[pl.ds(piece * piece_cols, piece_cols)]

    def grad_copy(way, piece, hop):
        where = piece_slice(ring.at(-step_of(way) * hop), piece)
        return pltpu.make_async_remote_copy(
            src_ref=gall.at[where] if hop else own_piece(piece), dst_ref=gall.at[where],
            send_sem=g_send.at[way, piece, hop], recv_sem=g_recv.at[way, piece, hop],
            device_id={"tp": ring.at(step_of(way))}, device_id_type=MESH,
        )

    def pair_copy(offset, piece):
        where = piece_slice(ring.at(offset), piece)
        g = offset % n
        return pltpu.make_async_remote_copy(
            src_ref=gall.at[where] if offset else own_piece(piece), dst_ref=mate.at[where],
            send_sem=p_send.at[g, piece], recv_sem=p_recv.at[g, piece],
            device_id=partner, device_id_type=MESH,
        )

    def gate_piece(piece):
        for way in range(2):
            sum_copy(way, piece, half - 1).wait_recv()
        for k in range(piece_cols):
            c = piece * piece_cols + k
            gate, up = (
                acc[part_at(0, c, m)]
                + blocks[landing(0, piece, half - 1) + k, :, side].astype(jnp.float32)
                + blocks[landing(1, piece, half - 1) + k, :, side].astype(jnp.float32)
                for m, side in enumerate((lower, upper))
            )
            s = jax.nn.sigmoid(gate)
            act = gate * s
            columns = slice(c * tile, (c + 1) * tile)
            cotangent = cot[:, columns].astype(jnp.float32)
            hid[:, columns] = (act * up).astype(jnp.bfloat16)
            own[c, :, lower] = (
                cotangent * up * (s * (1.0 + gate * (1.0 - s)))
            ).astype(jnp.bfloat16)
            own[c, :, upper] = (cotangent * act).astype(jnp.bfloat16)

    gate_piece(0)
    grad_copy(0, 0, 0).start()
    gate_piece(1)
    for way, piece in lanes[1:]:
        grad_copy(way, piece, 0).start()
    for piece in range(2):
        pair_copy(0, piece).start()
    hidden_copy = pltpu.make_async_copy(hid, hidden_ref, load_sem.at[3])
    hidden_copy.start()

    def clear(r):
        acc[r] = jnp.zeros(acc.shape[1:], acc.dtype)

    unrolled(tile_rows, clear)
    turned_copy.wait()

    def x_copy(i, off):
        _, start, size = chunks[i]
        dest = lax.rem(x_part + off, n_parts)
        return pltpu.make_async_remote_copy(
            src_ref=stage.at[i % n_stage, dest, pl.ds(0, size)],
            dst_ref=parts_ref.at[x_part, pl.ds(start, size)],
            send_sem=xs_send.at[i, off - 1], recv_sem=xs_recv.at[i, off - 1],
            device_id=x_device(off), device_id_type=MESH,
        )

    def keep_copy(i):
        _, start, size = chunks[i]
        return pltpu.make_async_copy(
            stage.at[i % n_stage, x_part, pl.ds(0, size)],
            parts_ref.at[x_part, pl.ds(start, size)],
            x_local.at[i],
        )

    def finish(i):
        for off in range(1, n_parts):
            x_copy(i, off).wait_send()
        keep_copy(i).wait()

    offsets = [0]
    for hop in range(1, half):
        offsets += [-hop, hop]
    offsets.append(half)
    side_blocks = cells * cols_dev

    def cell_of(offset):
        return offsets.index(offset) % cells * cols_dev

    def landed(step):
        return [offset for offset in offsets if abs(offset) == step]

    def fill(step, side):
        copies = []
        for number, offset in enumerate(landed(step)):
            for piece in range(2):
                if side:
                    pair_copy(offset, piece).wait_recv()
                    ref = mate.at[piece_slice(ring.at(offset), piece)]
                elif offset:
                    ref = gall.at[piece_slice(ring.at(offset), piece)]
                else:
                    ref = own_piece(piece)
                first = side * side_blocks + cell_of(offset) + piece * piece_cols
                copies.append(
                    pltpu.make_async_copy(
                        ref, blocks.at[pl.ds(first, piece_cols)],
                        work_sem.at[number, side, piece],
                    )
                )
                copies[-1].start()
        return copies

    def settle(copies):
        for copy in copies:
            copy.wait()

    def weight_grads(step, which=None):
        at_this = [i for i, chunk in enumerate(chunks) if chunk[0] == step]
        for i in at_this if which is None else at_this[which : which + 1]:
            _, start, size = chunks[i]
            if i >= n_stage:
                finish(i - n_stage)
            slot = i % n_stage

            def outer(j):
                r, block = tables[LIST_ROW, start + j], tables[LIST_BLOCK, start + j]
                value = jnp.dot(
                    xt[0, r], blocks[block], preferred_element_type=jnp.float32
                ) + jnp.dot(
                    xt[1, r], blocks[side_blocks + block], preferred_element_type=jnp.float32
                )
                for k in range(n_parts):
                    stage[slot, k, j] = value[k * band : (k + 1) * band].astype(jnp.bfloat16)

            unrolled(size, outer)
            for off in range(1, n_parts):
                x_copy(i, off).start()
            keep_copy(i).start()

    def token_grads(offset, source=None):
        shard = ring.at(offset)
        source = blocks if source is None else source
        cell = cell_of(offset) if source is blocks else shard * cols_dev
        buf[0] = jnp.zeros(buf.shape[1:], buf.dtype)
        for s, side in zip(range(n_seg), (lower, upper)):
            if s > 0:
                buf[0, :, side] = buf[seg, :, lower]

            def back(j):
                at = shard * list_len + s * seg + j
                term = lax.dot_general(
                    source[cell + tables[COL_B, at]], ww[tables[SLOT_B, at]],
                    (((1,), (1,)), ((), ())), preferred_element_type=jnp.float32,
                )
                kept = jnp.where(tables[KEEP_B, at] > 0, buf[j, :, side], 0.0)
                buf[j + 1, :, side] = term + kept

            unrolled(seg, back)

        def add_row(r):
            last = tables[LAST_B, shard * tile_rows + r]
            value = buf[jnp.minimum(last, seg), :, lower]
            if n_seg > 1:
                later = buf[jnp.maximum(last - seg, 0), :, upper]
                value = jnp.where(last > seg, later, value)
            acc[r] += value

        unrolled(tile_rows, add_row)

    def arrive(way, piece, hop):
        if hop >= hops(ring, way, piece):
            return
        grad_copy(way, piece, hop).wait_recv()
        if hop + 1 < hops(ring, way, piece):
            grad_copy(way, piece, hop + 1).start()
        pair_copy(-step_of(way) * (hop + 1), piece).start()

    settle(fill(0, 0))
    settle(fill(0, 1))
    weight_grads(0)
    token_grads(0)
    for hop in range(half - 1):
        arrive(0, 0, hop)
        arrive(1, 1, hop)
        if hop > 0:
            token_grads(-hop)
            token_grads(hop)
        arrive(0, 1, hop)
        arrive(1, 0, hop)
        settle(fill(hop + 1, 0) + fill(hop + 1, 1))
        if hop < half - 2:
            weight_grads(hop + 1)
    last = half - 1
    n_last = len([chunk for chunk in chunks if chunk[0] == last])
    n_half = len([chunk for chunk in chunks if chunk[0] == half])
    for which in range(n_last - 1):
        weight_grads(last, which)
    token_grads(-last)
    weight_grads(last, n_last - 1)
    token_grads(last)
    arrive(0, 0, last)
    arrive(1, 1, last)
    if big:
        settle(fill(half, 0))
        fills = []
        token_grads(half)
    else:
        fills = fill(half, 0)
        token_grads(half, gall)

    def d_copy(way, piece, hop):
        return pltpu.make_async_remote_copy(
            src_ref=dsend.at[way, piece, hop], dst_ref=drecv.at[way, piece, hop],
            send_sem=ds_send.at[way, piece, hop], recv_sem=ds_recv.at[way, piece, hop],
            device_id={"tp": ring.at(step_of(way))}, device_id_type=MESH,
        )

    def own_term(dest, piece):
        return acc[
            pl.ds(piece * fine_rows, fine_rows),
            pl.ds(pl.multiple_of(dest * rows, rows), rows),
            :,
        ]

    def d_first(way, piece):
        return half - fine_hops(ring, way, piece)

    def d_push(way, piece, hop):
        value = own_term(ring.at(step_of(way) * (half - hop)), piece)
        if hop > d_first(way, piece):
            d_copy(way, piece, hop - 1).wait_recv()
            value = value + drecv[way, piece, hop - 1].astype(jnp.float32)
        dsend[way, piece, hop] = value.astype(jnp.bfloat16)
        d_copy(way, piece, hop).start()

    for hop in range(half):
        fresh = [lane for lane in fine_lanes if hop == d_first(*lane)]
        going = [lane for lane in fine_lanes if hop > d_first(*lane)]
        for way, piece in fresh + going:
            d_push(way, piece, hop)
        if hop == 0:
            settle(fills + fill(half, 1))
        if hop < n_half:
            weight_grads(half, hop)
    for piece in range(FINE):
        for way in range(2):
            d_copy(way, piece, half - 1).wait_recv()
        d_ref[pl.ds(piece * fine_rows, fine_rows)] = (
            own_term(me, piece)
            + drecv[0, piece, half - 1].astype(jnp.float32)
            + drecv[1, piece, half - 1].astype(jnp.float32)
        ).astype(jnp.bfloat16)

    for i in range(max(0, len(chunks) - n_stage), len(chunks)):
        finish(i)
    for i in range(len(chunks)):
        for off in range(1, n_parts):
            x_copy(i, off).wait_recv()
    for way, piece in lanes:
        for hop in range(hops(ring, way, piece)):
            grad_copy(way, piece, hop).wait_send()
        for hop in range(max(first_hop(way, piece), half - 2), half):
            sum_copy(way, piece, hop).wait_send()
    for way, piece in fine_lanes:
        for hop in range(fine_hops(ring, way, piece)):
            token_copy(way, piece, hop).wait_send()
        for hop in range(d_first(way, piece), half):
            d_copy(way, piece, hop).wait_send()
    for offset in offsets:
        for piece in range(2):
            pair_copy(offset, piece).wait_send()
    hidden_copy.wait()


def step(slot_tile, normed, cotangent, weights, n, list_len, dp_size):
    rows, width = normed.shape
    owned, tile = weights.shape[1:3]
    tile_rows = width // tile
    tokens, cols = cotangent.shape
    cols_dev = cols // tile
    pair = 2 * tile
    half = n // 2
    band = tile // dp_size
    n_parts = dp_size // CORES
    n_stage = 4
    chunks, cells = plan = arrival_plan(n, owned)
    largest = max(size for _, _, size in chunks)
    dims = (n, tile_rows, cols_dev, list_len, rows, tokens, tile, dp_size, owned)
    hbm = pl.BlockSpec(memory_space=pl.ANY)
    vmem = pl.BlockSpec(memory_space=pltpu.VMEM)
    sem = pltpu.SemaphoreType.DMA
    gall_shape = (n * cols_dev, tokens, pair)
    big = n * cols_dev * tokens * pair * 2 > 12 * 2**20
    seg = list_len // 2 if list_len % 8 == 0 else list_len
    most = -(-max(n * list_len, n * tile_rows, owned) // tile) * tile
    d_slots = (2, FINE, half, tile_rows // FINE, rows, tile)
    out_specs = [hbm, vmem, hbm, vmem, hbm]
    out_shape = [
        jax.ShapeDtypeStruct((tokens, cols), jnp.bfloat16),
        jax.ShapeDtypeStruct((tile_rows, rows, tile), jnp.bfloat16),
        jax.ShapeDtypeStruct((n_parts, owned, band, pair), jnp.bfloat16),
        jax.ShapeDtypeStruct((1, owned), jnp.int32),
        jax.ShapeDtypeStruct(gall_shape, jnp.bfloat16),
    ]
    scratch = []
    if big:
        out_specs.append(hbm)
        out_shape.append(jax.ShapeDtypeStruct(gall_shape, jnp.bfloat16))
    else:
        scratch.append(pltpu.VMEM(gall_shape, jnp.bfloat16))
    n_blocks = max(4 * half * (cols_dev // 2), 2 * cells * cols_dev)
    scratch += [
        pltpu.VMEM((cols_dev, tokens, pair), jnp.bfloat16),
        pltpu.VMEM((tile_rows, tokens, tile), jnp.bfloat16),
        pltpu.VMEM((owned, tile, pair), jnp.bfloat16),
        pltpu.VMEM((seg + 1, tokens, pair), jnp.float32),
        pltpu.VMEM((max(4 * cols_dev, tile_rows), tokens, tile), jnp.float32),
        pltpu.VMEM((2, 2, 2, cols_dev // 2, tokens, pair), jnp.bfloat16),
        pltpu.VMEM((n_blocks, tokens, pair), jnp.bfloat16),
        pltpu.VMEM((3, tile_rows, tile // CORES, tokens), jnp.bfloat16),
        pltpu.VMEM((n_stage, n_parts, largest, band, pair), jnp.bfloat16),
        pltpu.VMEM(d_slots, jnp.bfloat16),
        pltpu.VMEM(d_slots, jnp.bfloat16),
        pltpu.VMEM((tokens, cols), jnp.bfloat16),
        pltpu.VMEM((tokens, cols), jnp.bfloat16),
        pltpu.VMEM((8, owned), jnp.int32),
        pltpu.VMEM((16, most), jnp.int32),
        pltpu.SMEM((16, most), jnp.int32),
        sem((tile_rows,)), sem((4,)), sem((1,)),
        sem((2, FINE, half)), sem((2, FINE, half)), sem((2, 2, half)), sem((2, 2, half)),
        sem((2, 2, 2)), sem((2, 2, half)), sem((2, 2, half)),
        sem((n, 2)), sem((n, 2)), sem((2,)),
        sem((len(chunks), n_parts - 1)), sem((len(chunks), n_parts - 1)), sem((len(chunks),)),
        sem((2, FINE, half)), sem((2, FINE, half)),
    ]
    results = pl.pallas_call(
        functools.partial(step_kernel, dims, plan, big),
        name="step",
        in_specs=[vmem, hbm, hbm, hbm],
        out_specs=out_specs,
        out_shape=out_shape,
        scratch_shapes=scratch,
        compiler_params=pltpu.CompilerParams(
            collective_id=0, has_side_effects=True, vmem_limit_bytes=VMEM_LIMIT
        ),
    )(slot_tile.reshape(1, -1), normed, cotangent, weights)
    return results[:4]


def finish_kernel(place_ref, parts_ref, d_ref, hidden_ref, out_ref, d_out, hidden_out):
    n_parts = parts_ref.shape[0]
    _, chunk, _, tile = out_ref.shape
    base = pl.program_id(0) * chunk

    @pl.when(pl.program_id(0) == 0)
    def _():
        for r in range(d_ref.shape[0]):
            d_out[:, r * tile : (r + 1) * tile] = d_ref[r]

    hidden_out[...] = hidden_ref[...]

    def one(p):
        at = place_ref[base + p]
        total = parts_ref[0, at].astype(jnp.float32)
        for k in range(1, n_parts):
            total = total + parts_ref[k, at].astype(jnp.float32)
        out_ref[0, p] = total[:, :tile]
        out_ref[1, p] = total[:, tile:]

    unrolled(chunk, one)


def finish_sum(place, parts, d, hidden):
    owned = place.shape[0]
    n_parts, listed, band, pair = parts.shape
    tile = pair // 2
    tile_rows, rows, _ = d.shape
    tokens, cols = hidden.shape
    steps = 2
    return pl.pallas_call(
        finish_kernel,
        name="finish",
        grid=(steps,),
        in_specs=[
            pl.BlockSpec(memory_space=pltpu.SMEM),
            pl.BlockSpec((n_parts, listed, band, pair), lambda i: (0, 0, 0, 0)),
            pl.BlockSpec((tile_rows, rows, tile), lambda i: (0, 0, 0)),
            pl.BlockSpec((tokens // steps, cols), lambda i: (i, 0)),
        ],
        out_specs=[
            pl.BlockSpec((2, owned // steps, band, tile), lambda i: (0, i, 0, 0)),
            pl.BlockSpec((rows, tile_rows * tile), lambda i: (0, 0)),
            pl.BlockSpec((tokens // steps, cols), lambda i: (i, 0)),
        ],
        out_shape=[
            jax.ShapeDtypeStruct((2, owned, band, tile), jnp.float32),
            jax.ShapeDtypeStruct((rows, tile_rows * tile), d.dtype),
            jax.ShapeDtypeStruct(hidden.shape, hidden.dtype),
        ],
        compiler_params=pltpu.CompilerParams(vmem_limit_bytes=VMEM_LIMIT),
    )(place, parts, d, hidden)


def local(normed, cotangent, weight_tiles, slot_tile):
    n = lax.axis_size("tp")
    dp_size = lax.axis_size("dp")
    owned = weight_tiles.shape[1]
    base_count = owned // n
    list_len = base_count + base_count // 4
    hidden, d, parts, rank = step(
        slot_tile, normed, cotangent, weight_tiles, n, list_len, dp_size
    )
    grad_tiles, d_normed, hidden = finish_sum(rank.reshape(owned), parts, d, hidden)
    return hidden, d_normed, grad_tiles


def solution(mesh):
    return jax.shard_map(
        local,
        mesh=mesh,
        in_specs=(P(("dp", "tp"), None), P("dp", "tp"), P(None, "tp", None, None), P()),
        out_specs=(P("dp", "tp"), P(("dp", "tp"), None), P(None, "tp", "dp", None)),
        check_vma=False,
    )
```
